32 devices in a mesh: tm: 2 (over core), stn: 4 (over z), chan: 4 (over y, x).
Axes of the slice: x: 2, y: 2, z: 4, core: 2. Of those that a mesh axis runs over, the one named last changes fastest.
Arguments:
- voltages: bfloat16 [2, 8, 512, 32, 2, 256], P(None, 'chan', 'stn', 'tm'), may hold values from -100 to 100
- fir_taps: float32 [16, 256], replicated, may hold values from -1.5 to 1.5
- station_map: int32 [512], P('stn'), may hold values from 0 to 31, as said below
- beam_index: int32 [512], P('stn'), may hold values from 0 to 15
- weight_table: bfloat16 [2, 16, 8, 8], P(None, None, 'chan'), may hold values from -1.5 to 1.5
Outputs:
- visibilities: float32 [2, 2, 8, 32, 32, 8, 2, 2, 256], P('tm', None, 'chan', 'stn')
The draws below stay inside these ranges and needn't reach their ends.
Inputs may be any that keep to these rules, and one draw needn't show every extreme that they name: `station_map`: each station number names exactly 16 dishes; of the dishes g * 128 up to (g + 1) * 128 - 1, exactly 32 name a station of the block h * 8 up to (h + 1) * 8 - 1, for every g and h.
All inputs are finite; a program needn't handle non-finite values.
Results may differ from the reference program's by a relative error of at most 0.017.
Values may be sent and summed in bfloat16 or wider, within the bound.
No kernel may reach another device: no remote copies, remote signals or barrier semaphores. Data moves between devices by JAX's collectives and lax.ppermute only.
A program may use at most 512 MiB of HBM per device.

```python
import jax
import jax.numpy as jnp
from jax import lax

DISHES = 512
STATIONS = 32
DPS = 16
BEAMS = 8
POL = 2
COARSE = 8
FINE = 256
TAPS = 16
NTAB = 16
FRAMES_DEV = 16
FRAMES = 32
N_TM = 2
N_STN = 4


def draw_voltages(key, part):
    noise_key, sample_key, frame_key = jax.random.split(jax.random.fold_in(key, 11), 3)
    shape = (2, COARSE, DISHES, FRAMES, POL, FINE)
    noise_draw = jnp.clip(jax.random.normal(noise_key, shape, jnp.float32), -6.0, 6.0)
    rise_factor = 3.0
    coarse_pos = jnp.arange(COARSE, dtype=jnp.float32) / max(COARSE - 1, 1)
    coarse_amp = jnp.sqrt(rise_factor ** coarse_pos)
    sample_amp = 10.0 ** (0.5 * jax.random.uniform(sample_key, (FINE,), jnp.float32))
    frame_amp = 3.0 ** (0.5 * jax.random.uniform(frame_key, (FRAMES,), jnp.float32))
    scaled = noise_draw * coarse_amp[None, :, None, None, None, None] * frame_amp[None, None, None, :, None, None] * sample_amp
    return scaled.astype(jnp.bfloat16)


def draw_station_map(key, part):
    group_dishes = DISHES // N_STN
    share = group_dishes // N_STN
    owned = STATIONS // N_STN
    first_key, second_key = jax.random.split(jax.random.fold_in(key, 23), 2)
    base = jnp.arange(group_dishes, dtype=jnp.int32)
    ranks = jax.vmap(lambda sub_key: jax.random.permutation(sub_key, base))(jax.random.split(first_key, N_STN))
    placing = jax.vmap(lambda sub_key: jax.random.permutation(sub_key, base))(jax.random.split(second_key, N_STN))
    owner = ranks // share
    group_ids = jnp.arange(N_STN, dtype=jnp.int32)[:, None]
    column = group_ids * share + ranks % share
    position = placing[owner, column]
    station = owner * owned + position // (DISHES // STATIONS)
    return station.reshape(DISHES).astype(jnp.int32)


def place_ends(values, stream_key, least, largest):
    dims = values.shape
    index_at = [jax.random.randint(jax.random.fold_in(stream_key, axis), (), 0, dims[axis]) for axis in range(len(dims))]
    values = values.at[tuple(index_at)].set(least)
    longest = dims.index(max(dims))
    index_at[longest] = (index_at[longest] + 1) % dims[longest]
    return values.at[tuple(index_at)].set(largest)


def level_of(key, shape, cuts, smallest, largest):
    def one(dim, blocks):
        heights = jax.random.uniform(jax.random.fold_in(jax.random.fold_in(key, 6), dim), (blocks,), jnp.float32, smallest / len(cuts), largest / len(cuts))
        return jnp.repeat(jnp.exp(heights), shape[dim] // blocks).reshape((-1,) + (1,) * (len(shape) - dim - 1))

    level = one(*cuts[0])
    for cut in cuts[1:]:
        level = level * one(*cut)
    return level


def bell_draw(rng, shape, deviation, most, pieces=(), kind=jnp.bfloat16):
    level = level_of(rng, shape, pieces, -0.22, 0.18) if pieces else 1.0
    array = jax.random.normal(rng, shape, jnp.float32) * deviation * level
    return jnp.minimum(jnp.maximum(array, -most), most).astype(kind)


def setup_inputs(seed: int = 0) -> dict:
    seeds = jax.random.split(jax.random.key(seed), 6)
    voltages = draw_voltages(jax.random.fold_in(seeds[5], 71), 0)
    fir_taps = bell_draw(seeds[1], (TAPS, FINE), TAPS ** -0.5, 1.5, (), jnp.float32)
    station_map = draw_station_map(jax.random.fold_in(seeds[5], 71), 0)
    beam_index = place_ends(jax.random.randint(seeds[3], (DISHES,), 0, NTAB), jax.random.fold_in(seeds[3], 1), 0, NTAB - 1).astype(jnp.int32)
    weight_table = bell_draw(seeds[4], (2, NTAB, COARSE, BEAMS), DPS ** -0.5, 1.5, ((2, 4),))
    return {"voltages": voltages, "fir_taps": fir_taps, "station_map": station_map, "beam_index": beam_index, "weight_table": weight_table}


epsilon = 1e-06

def dft_tables(length):
    bin_index = jnp.arange(length, dtype=jnp.int32)
    phase_step = bin_index[:, None] * bin_index[None, :] % length
    angles = phase_step.astype(jnp.float32) * (2.0 * jnp.pi / length)
    return (jnp.cos(angles).astype(jnp.bfloat16), jnp.sin(angles).astype(jnp.bfloat16))

def correlate(normed_slice):
    values = normed_slice.astype(jnp.float32)
    real_part = values[:, 0]
    imag_part = values[:, 1]

    def product(left_beams, right_beams):
        return jnp.einsum('sbfpk,tbfqk->stbpqk', left_beams, right_beams)
    vis_re = product(real_part, real_part) + product(imag_part, imag_part)
    vis_im = product(imag_part, real_part) - product(real_part, imag_part)
    return jnp.stack([vis_re, vis_im]) / FRAMES_DEV

def reference(voltages, fir_taps, station_map, beam_index, weight_table):
    cosine, sine_table = dft_tables(FINE)
    history = TAPS - 1
    group_size = DISHES // N_STN
    station_hot = (station_map[:, None] == jnp.arange(STATIONS, dtype=jnp.int32)[None, :]).astype(jnp.float32)
    table_hot = (beam_index[:, None] == jnp.arange(NTAB, dtype=jnp.int32)[None, :]).astype(jnp.float32)

    def channel_beams(inputs):
        samples, table_slice = inputs
        padded = jnp.pad(samples, ((0, 0), (0, 0), (history, 0), (0, 0), (0, 0)))
        filtered = jnp.zeros(samples.shape, jnp.float32)
        for tap_index in range(TAPS):
            offset = history - tap_index
            filtered = filtered + fir_taps[tap_index] * padded[:, :, offset:offset + FRAMES].astype(jnp.float32)
        filtered = filtered.astype(jnp.bfloat16)
        real_part = filtered[0].reshape(-1, FINE)
        imag_part = filtered[1].reshape(-1, FINE)
        spec_re = jnp.dot(real_part, cosine, preferred_element_type=jnp.float32) + jnp.dot(imag_part, sine_table, preferred_element_type=jnp.float32)
        spec_im = jnp.dot(imag_part, cosine, preferred_element_type=jnp.float32) - jnp.dot(real_part, sine_table, preferred_element_type=jnp.float32)
        spectra_low = jnp.stack([spec_re, spec_im]).reshape(samples.shape).astype(jnp.bfloat16)
        spectra = lax.optimization_barrier(spectra_low).astype(jnp.float32)
        weights = jnp.einsum('dt,otb->odb', table_hot, table_slice.astype(jnp.float32))
        weight_re = weights[0]
        weight_im = weights[1]
        mixing = jnp.stack([jnp.stack([weight_re, -weight_im]), jnp.stack([weight_im, weight_re])])
        steering = station_hot[None, None, :, :, None] * mixing[:, :, :, None, :]
        summed = jnp.zeros((STATIONS, 2, BEAMS, FRAMES, POL, FINE), jnp.float32)
        for dish_group in range(N_STN):
            low_dish = dish_group * group_size
            partial_value = jnp.einsum('oidsb,idfpk->sobfpk', steering[:, :, low_dish:low_dish + group_size], spectra[:, low_dish:low_dish + group_size])
            rounded = lax.optimization_barrier(partial_value.astype(jnp.bfloat16))
            summed = summed + rounded.astype(jnp.float32)
        return summed.astype(jnp.bfloat16)
    formed = lax.map(channel_beams, (jnp.moveaxis(voltages, 1, 0), jnp.moveaxis(weight_table, 2, 0)))
    outputs = []
    for time_block in range(N_TM):
        first_frame = time_block * FRAMES_DEV
        values = formed[:, :, :, :, first_frame:first_frame + FRAMES_DEV].astype(jnp.float32)
        power_sum = lax.optimization_barrier(jnp.sum(values * values, axis=(0, 2, 4, 6)))
        inverse_rms = lax.rsqrt(power_sum / (COARSE * FRAMES_DEV * FINE) + epsilon)
        normed = (values * inverse_rms[None, :, None, :, None, :, None]).astype(jnp.bfloat16)
        visibility = lax.map(correlate, normed)
        outputs.append(jnp.moveaxis(visibility, 0, 1))
    return jnp.stack(outputs)
```

```python
import jax
import jax.numpy as jnp
from jax import lax
from jax.experimental import pallas as pl
from jax.experimental.pallas import tpu as pltpu
from jax.sharding import PartitionSpec as P


STATIONS = 32
COARSE = 8
LANES = 128
UNROLL = 8
PREPARE = 4
PAIRS = (2, 4)

epsilon = 1e-06


def shifted(value, axis, steps):
    count = lax.axis_size(axis)
    first, last = (max(0, -steps), min(count, count - steps))
    return lax.ppermute(value, axis, [(source, source + steps) for source in range(first, last)])


def dft_tables(length):
    bin_index = jnp.arange(length, dtype=jnp.int32)
    phase_step = bin_index[:, None] * bin_index[None, :] % length
    angles = phase_step.astype(jnp.float32) * (2.0 * jnp.pi / length)
    return (jnp.cos(angles).astype(jnp.bfloat16), jnp.sin(angles).astype(jnp.bfloat16))


def block_ranks(station_map, block_stations, share):
    block = station_map // block_stations
    position = jnp.arange(station_map.shape[-1], dtype=jnp.int32)
    same = block[..., :, None] == block[..., None, :]
    before = position[None, :] < position[:, None]
    return block * share + jnp.sum((same & before).astype(jnp.int32), axis=-1)


def sort_dishes(voltages, order, coarse, parts, share):
    comps, _, _, frames, pols, fine = voltages.shape
    tiles = fine // LANES

    def body(order_ref, x_ref, *refs):
        outs, sems = refs[: len(parts)], refs[len(parts) :]

        def issue(place, carry):
            for part, out_ref, sem in zip(parts, outs, sems):
                dish = order_ref[part * share + place]
                for tile in range(tiles):
                    lanes = pl.ds(tile * LANES, LANES)
                    pltpu.make_async_copy(
                        x_ref.at[:, coarse, dish, :, :, lanes], out_ref.at[:, :, tile, place], sem
                    ).start()
            return carry

        lax.fori_loop(0, share, issue, 0)
        for out_ref, sem in zip(outs, sems):
            pltpu.make_async_copy(out_ref, out_ref, sem).wait()

    results = pl.pallas_call(
        body,
        out_shape=[jax.ShapeDtypeStruct((comps, frames, tiles, share, pols, LANES), voltages.dtype)] * len(parts),
        in_specs=[pl.BlockSpec(memory_space=pltpu.SMEM), pl.BlockSpec(memory_space=pl.ANY)],
        out_specs=[pl.BlockSpec(memory_space=pltpu.VMEM)] * len(parts),
        scratch_shapes=[pltpu.SemaphoreType.DMA] * len(parts),
        name="sort_dishes",
    )(order, voltages)

    return [array.reshape(comps, frames, tiles, share * pols, LANES) for array in results]


def beam_sums(weights, sources, frames_step=4):
    comps, frames, tiles, rows, _ = sources[0].shape
    out_rows, contract = weights.shape

    def body(w_ref, *refs):
        out_ref = refs[-1]
        for frame in range(frames_step):
            pieces = []
            for ref in refs[:-1]:
                for comp in range(comps):
                    pieces.append(jnp.concatenate([ref[comp, frame, t] for t in range(tiles)], axis=1))
            stacked = jnp.concatenate(pieces, axis=0)
            out_ref[frame] = jnp.dot(
                w_ref[...], stacked, preferred_element_type=jnp.float32
            ).astype(out_ref.dtype)

    return pl.pallas_call(
        body,
        grid=(frames // frames_step,),
        in_specs=[pl.BlockSpec((out_rows, contract), lambda i: (0, 0))]
        + [pl.BlockSpec((comps, frames_step, tiles, rows, LANES), lambda i: (0, i, 0, 0, 0))] * len(sources),
        out_specs=pl.BlockSpec((frames_step, out_rows, tiles * LANES), lambda i: (i, 0, 0)),
        out_shape=jax.ShapeDtypeStruct((frames, out_rows, tiles * LANES), jnp.bfloat16),
        name="beam_sums",
    )(weights, *sources)


def channelize(previous, current, taps, cosine, sine, beams):
    frames, out_rows, fine = current.shape
    taps_count = taps.shape[0]
    history = taps_count - 1
    rows = out_rows // (2 * beams)
    tiles = fine // LANES
    previous = previous.reshape(frames, 2, beams * rows, fine)
    current = current.reshape(frames, 2, beams * rows, fine)
    wide_taps = jnp.broadcast_to(taps[:, None, :], (taps_count, 8, fine))

    def body(prev_ref, cur_ref, taps_ref, cos_ref, sin_ref, out_ref, pow_ref, wide_ref, filt_ref):
        for frame in range(history):
            wide_ref[frame] = prev_ref[frames - history + frame].astype(jnp.float32)
        for frame in range(frames):
            wide_ref[history + frame] = cur_ref[frame].astype(jnp.float32)
        for comp in range(2):
            for tile in range(tiles):
                lanes = slice(tile * LANES, (tile + 1) * LANES)
                for low in range(0, rows, 8):
                    for frame in range(frames):
                        terms = [
                            taps_ref[tap, :, lanes]
                            * wide_ref[history + frame - tap, comp, low : low + 8, lanes]
                            for tap in range(taps_count)
                        ]
                        while len(terms) > 1:
                            terms = [
                                a + b for a, b in zip(terms[::2], terms[1::2])
                            ] + terms[len(terms) // 2 * 2 :]
                        filt_ref[comp, frame * rows + low : frame * rows + low + 8, lanes] = terms[0]
        real_part = filt_ref[0].astype(jnp.bfloat16)
        imag_part = filt_ref[1].astype(jnp.bfloat16)

        def dot(a, b):
            return jnp.dot(a, b, preferred_element_type=jnp.float32)

        spec_re = dot(real_part, cos_ref[...]) + dot(imag_part, sin_ref[...])
        spec_im = dot(imag_part, cos_ref[...]) - dot(real_part, sin_ref[...])
        power = jnp.zeros((rows, LANES), jnp.float32)
        for comp, spectrum in enumerate((spec_re, spec_im)):
            rounded = spectrum.astype(jnp.bfloat16)
            squares = rounded.astype(jnp.float32)
            squares = squares * squares
            for tile in range(tiles):
                lanes = slice(tile * LANES, (tile + 1) * LANES)
                for frame in range(frames):
                    out_ref[0, comp, frame, tile * rows : (tile + 1) * rows, :] = rounded[
                        frame * rows : (frame + 1) * rows, lanes
                    ]
                    power = power + squares[frame * rows : (frame + 1) * rows, lanes]
        pow_ref[0] = power

    return pl.pallas_call(
        body,
        grid=(beams,),
        in_specs=[
            pl.BlockSpec((frames, 2, rows, fine), lambda b: (0, 0, b, 0)),
            pl.BlockSpec((frames, 2, rows, fine), lambda b: (0, 0, b, 0)),
            pl.BlockSpec((taps_count, 8, fine), lambda b: (0, 0, 0)),
            pl.BlockSpec((fine, fine), lambda b: (0, 0)),
            pl.BlockSpec((fine, fine), lambda b: (0, 0)),
        ],
        out_specs=[
            pl.BlockSpec((1, 2, frames, tiles * rows, LANES), lambda b: (b, 0, 0, 0, 0)),
            pl.BlockSpec((1, rows, LANES), lambda b: (b, 0, 0)),
        ],
        out_shape=[
            jax.ShapeDtypeStruct((beams, 2, frames, tiles * rows, LANES), jnp.bfloat16),
            jax.ShapeDtypeStruct((beams, rows, LANES), jnp.float32),
        ],
        scratch_shapes=[
            pltpu.VMEM((history + frames, 2, rows, fine), jnp.float32),
            pltpu.VMEM((2, frames * rows, fine), jnp.float32),
        ],
        name="channelize",
    )(previous, current, wide_taps, cosine, sine)


def spread_matrix(stations, pols, tiles, left):
    shape = (stations, pols, tiles, pols)
    station, p, tile, q = (lax.broadcasted_iota(jnp.int32, shape, axis).reshape(-1) for axis in range(4))
    source = (tile * stations + station) * pols + (p if left else q)
    column = jnp.arange(tiles * stations * pols, dtype=jnp.int32)
    return (source[:, None] == column[None, :]).astype(jnp.bfloat16)


def correlate(out, left, rights, left_scale, right_scale, coarse, coarse_count, block, pols):
    beams, _, frames, rows, _ = left.shape
    _, own, unit, _ = left_scale.shape
    stations = right_scale.shape[1]
    tiles = unit // (pols * pols)
    blocks = len(rights)
    others = own * blocks
    size = own * unit
    spread_left = spread_matrix(own, pols, tiles, True)
    spread_right = spread_matrix(own, pols, tiles, False)
    pair_left, pair_right = PAIRS
    choice = [right if isinstance(right, tuple) else (right,) for right in rights]
    flag = next((right[2] for right in choice if len(right) == 3), 0)
    arrays = [array for right in choice for array in right[:2]]
    scalars = jnp.stack([jnp.asarray(block, jnp.int32), jnp.asarray(flag, jnp.int32)])

    def body(scalar_ref, *refs):
        left_ref, sl_ref, pl_ref, pr_ref = refs[:4]
        right_refs = list(refs[4 : 4 + len(arrays)])
        sr_ref = refs[4 + len(arrays)]
        out_ref, l_ref, r_ref = refs[-3:]

        def spread(matrix_ref, pieces, scale):
            wide = jnp.dot(
                matrix_ref[...], jnp.concatenate(pieces, axis=1), preferred_element_type=jnp.float32
            )
            return [wide[:, i * LANES : (i + 1) * LANES] * scale for i in range(len(pieces))]

        def chosen(index, frame):
            place = sum(min(len(c), 2) for c in choice[:index])
            halves = [right_refs[place][0, o, frame] for o in range(2)]
            if len(choice[index]) == 3:
                second = right_refs[place + 1]
                halves = [jnp.where(scalar_ref[1] == 0, halves[o], second[0, o, frame]) for o in range(2)]
            return halves

        span = PREPARE
        left_scales = sl_ref[0].reshape(size, LANES)
        for first in range(0, frames, span):
            those = range(first, first + span)
            parts = spread(pl_ref, [left_ref[0, o, f] for f in those for o in range(2)], left_scales)
            for frame in those:
                real, imag = parts[2 * (frame - first)], parts[2 * (frame - first) + 1]
                l_ref[frame, 0] = real
                l_ref[frame, 1] = imag
                l_ref[frame, 2] = real + imag
        for index in range(blocks):
            low, high = index * size, (index + 1) * size
            scale = sr_ref[0, index * own : (index + 1) * own].reshape(size, LANES)
            for first in range(0, frames, span):
                those = range(first, first + span)
                parts = spread(pr_ref, [half for f in those for half in chosen(index, f)], scale)
                for frame in those:
                    real, imag = parts[2 * (frame - first)], parts[2 * (frame - first) + 1]
                    r_ref[frame, 0, low:high] = real
                    r_ref[frame, 1, low:high] = imag
                    r_ref[frame, 2, low:high] = real - imag

        left_groups = own // pair_left

        def products(step, carry):
            first_left = (step % left_groups) * pair_left
            first_right = (step // left_groups) * pair_right
            pairs = [(i, j) for i in range(pair_left) for j in range(pair_right)]

            def add_frame(frame, sums):
                lefts = [
                    [l_ref[frame, k, pl.ds((first_left + i) * unit, unit)] for k in range(3)]
                    for i in range(pair_left)
                ]
                result = []
                for j in range(pair_right):
                    right = [r_ref[frame, k, pl.ds((first_right + j) * unit, unit)] for k in range(3)]
                    for i in range(pair_left):
                        for k in range(3):
                            result.append(sums[(j * pair_left + i) * 3 + k] + lefts[i][k] * right[k])
                return tuple(result)

            zeros = tuple(jnp.zeros((unit, LANES), jnp.float32) for _ in range(3 * len(pairs)))
            sums = lax.fori_loop(0, frames, add_frame, zeros, unroll=UNROLL)
            for i, j in pairs:
                rr, ii, mixed = sums[(j * pair_left + i) * 3 : (j * pair_left + i) * 3 + 3]
                out_ref[0, 0, first_left + i, first_right + j, 0] = rr + ii
                out_ref[1, 0, first_left + i, first_right + j, 0] = mixed - rr + ii
            return carry

        lax.fori_loop(0, left_groups * (others // pair_right), products, 0)

    beam_spec = pl.BlockSpec((1, 2, frames, rows, LANES), lambda b, s: (b, 0, 0, 0, 0))
    operands = [left, left_scale, spread_left, spread_right, *arrays, right_scale]
    in_specs = [
        beam_spec,
        pl.BlockSpec((1, own, unit, LANES), lambda b, s: (b, 0, 0, 0)),
        pl.BlockSpec(spread_left.shape, lambda b, s: (0, 0)),
        pl.BlockSpec(spread_right.shape, lambda b, s: (0, 0)),
        *[beam_spec for _ in arrays],
        pl.BlockSpec((1, others, unit, LANES), lambda b, s: (b, s[0] // blocks, 0, 0)),
    ]
    aliases = {}
    if out is not None:
        aliases = {1 + len(operands): 0}
        operands.append(out)
        in_specs.append(pl.BlockSpec(memory_space=pl.ANY))
    shape = (2, coarse_count, own, stations, beams, unit, LANES)
    return pl.pallas_call(
        body,
        grid_spec=pltpu.PrefetchScalarGridSpec(
            num_scalar_prefetch=1,
            grid=(beams,),
            in_specs=in_specs,
            out_specs=pl.BlockSpec(
                (2, 1, own, others, 1, unit, LANES), lambda b, s: (0, coarse, 0, s[0] // blocks, b, 0, 0)
            ),
            scratch_shapes=[
                pltpu.VMEM((frames, 3, size, LANES), jnp.float32),
                pltpu.VMEM((frames, 3, others * unit, LANES), jnp.float32),
            ],
        ),
        out_shape=jax.ShapeDtypeStruct(shape, jnp.float32),
        input_output_aliases=aliases,
    )(scalars, *operands)


def block_weights(maps, weight_table, target, block_stations, share, pols):
    stations, rows = maps[:, 0], maps[:, 1]
    groups = maps.shape[0]
    _, table_rows, coarse, beams = weight_table.shape
    ranks = block_ranks(stations, block_stations, share)
    place = target * share + jnp.arange(share, dtype=jnp.int32)
    chosen = ranks[:, None, :] == place[None, :, None]
    station = jnp.sum(jnp.where(chosen, stations[:, None, :], 0), axis=-1) - target * block_stations
    row = jnp.sum(jnp.where(chosen, rows[:, None, :], 0), axis=-1)
    columns = (groups, 2, share, pols)
    out_rows = (2, beams, block_stations, pols)
    station = jnp.broadcast_to(station[:, None, :, None], columns).reshape(1, -1)
    row = jnp.broadcast_to(row[:, None, :, None], columns).reshape(1, -1)
    part, pol = (lax.broadcasted_iota(jnp.int32, columns, axis).reshape(1, -1) for axis in (1, 3))
    own_station, own_pol = (lax.broadcasted_iota(jnp.int32, out_rows, axis).reshape(-1, 1) for axis in (2, 3))
    term = jnp.arange(2 * table_rows, dtype=jnp.int32)[:, None]
    hot = (term == part * table_rows + row).astype(jnp.bfloat16)
    kept = (station == own_station) & (pol == own_pol)
    real, imag = weight_table[0], weight_table[1]
    mixing = jnp.stack([jnp.concatenate([real, -imag]), jnp.concatenate([imag, real])])
    result = []
    for channel in range(coarse):
        table = mixing[:, :, channel].swapaxes(1, 2)[:, :, None, None]
        table = jnp.broadcast_to(table, out_rows + (2 * table_rows,)).reshape(-1, 2 * table_rows)
        values = jnp.dot(table, hot, preferred_element_type=jnp.float32)
        result.append(jnp.where(kept, values, 0.0).astype(jnp.bfloat16))
    return result


def scales(power, denominator, frames, own_index, tiles):
    inverse = lax.rsqrt(power / denominator + epsilon)
    blocks, beams, own_count, pols = inverse.shape
    inverse = jnp.moveaxis(inverse, 1, 0).reshape(beams, blocks * own_count, pols)
    full = (beams, blocks * own_count, pols, tiles, pols, LANES)
    unit = pols * tiles * pols
    right = jnp.broadcast_to(inverse[:, :, None, None, :, None] / frames, full)
    mine = lax.dynamic_slice_in_dim(inverse, own_index * own_count, own_count, 1)
    left = jnp.broadcast_to(mine[:, :, :, None, None, None], (beams, own_count) + full[2:])
    return left.reshape(beams, own_count, unit, LANES), right.reshape(beams, blocks * own_count, unit, LANES)


def per_device(voltages, fir_taps, station_map, beam_index, weight_table):
    _, coarse_dev, dishes_dev, frames, pols, fine = voltages.shape
    groups = lax.axis_size("stn")
    own_index = lax.axis_index("stn")
    beams = weight_table.shape[3]
    share = dishes_dev // groups
    own_count = STATIONS // groups
    tiles = fine // LANES
    denominator = COARSE * frames * fine
    cosine, sine = dft_tables(fine)
    places = jnp.arange(dishes_dev, dtype=jnp.int32)
    line = groups == 4
    side = own_index // 2 if line else 0
    ranks = block_ranks(station_map, own_count, share)
    ranks = (ranks + 2 * side * share) % dishes_dev
    order = jnp.sum(jnp.where(ranks[None, :] == places[:, None], places[None, :], 0), axis=1)
    maps = jnp.stack([station_map, beam_index])

    def form(weights, sources):
        sums = beam_sums(weights, sources)
        earlier = shifted(sums, "tm", 1)
        formed, lane_power = channelize(earlier, sums, fir_taps, cosine, sine, beams)
        return formed, jnp.sum(lane_power, axis=-1)

    def place_power(power):
        return power.reshape(groups, beams, own_count, pols)

    out = None
    if not line:
        maps = lax.all_gather(maps, "stn")
        weights = block_weights(maps, weight_table, own_index, own_count, share, pols)
        formed, power = [], 0.0
        for coarse in range(coarse_dev):
            blocks = jnp.stack(sort_dishes(voltages, order, coarse, range(groups), share))
            arrived = lax.all_to_all(blocks, "stn", 0, 0, tiled=True)
            own, more = form(weights[coarse], [arrived[g] for g in range(groups)])
            power = power + more
            formed.append((own, lax.all_gather(own, "stn")))
        power = place_power(lax.psum(lax.all_gather(power, "stn"), "chan"))
        left_scale, right_scale = scales(power, denominator, frames, own_index, tiles)
        for coarse in range(coarse_dev):
            own, everyone = formed[coarse]
            rights = [everyone[g] for g in range(groups)]
            out = correlate(out, own, rights, left_scale, right_scale, coarse, coarse_dev, 0, pols)
    else:
        inward, across, outward = [(0, 1), (3, 2)], [(1, 2), (2, 1)], [(1, 0), (2, 3)]
        beyond_one = [(0, 2), (3, 1)]
        inner = (own_index == 1) | (own_index == 2)
        paths = (inward, across, beyond_one)
        known = [maps]
        for path in paths:
            known.append(lax.ppermute(maps, "stn", path))
        maps = jnp.stack(known)
        weights = [
            block_weights(maps, weight_table, 2 * side + step, own_count, share, pols) for step in range(2)
        ]
        steps = [(coarse, step) for coarse in range(coarse_dev) for step in range(2)]
        arrived = []
        for coarse, step in steps:
            index = len(arrived)
            near, far = sort_dishes(voltages, order, coarse, (step, 2 + step), share)
            sources = [near]
            for sent, path in zip((near, far, far), paths):
                sources.append(lax.ppermute(sent, "stn", path))
            arrived.append(sources)
        formed, ends, power = [], [], [0.0, 0.0]
        crossed = [None] * len(steps)
        for index, (coarse, step) in enumerate(steps):
            sources = arrived[index]
            if index:
                _, sources = lax.optimization_barrier((formed[-1], sources))
            own, more = form(weights[step][coarse], sources)
            formed.append(own)
            power[step] = power[step] + more
            ends.append(lax.ppermute(own, "stn", outward))
            if index == 0:
                crossed[0] = lax.ppermute(own, "stn", across)
        power = lax.psum(jnp.stack(power), "chan")
        beyond = lax.ppermute(power, "stn", across)
        beyond, *held = lax.optimization_barrier((beyond, *formed[1:]))
        for index, value in enumerate(held):
            crossed[index + 1] = lax.ppermute(value, "stn", across)
        both = jnp.stack([power, beyond])
        from_inner = lax.ppermute(both, "stn", outward)
        flag = jnp.where(inner, 0, 1)
        odd = own_index % 2 == 1
        from_inner, crossed[0] = lax.optimization_barrier((from_inner, crossed[0]))
        both = jnp.where(inner, both, from_inner)
        power = jnp.where(side == 0, both, both[::-1]).reshape((groups,) + power.shape[1:])
        left_scale, right_scale = scales(place_power(power), denominator, frames, own_index, tiles)
        far_ends, lefts = [], []

        def forward(index):
            far_ends.append(lax.ppermute(crossed[index], "stn", outward))

        def far_part(out, index):
            coarse, step = steps[index]
            far = [(crossed[index], far_ends[index], flag)]
            return correlate(
                out, lefts[coarse], far, left_scale, right_scale, coarse, coarse_dev,
                2 * (1 - side) + step, pols,
            )

        forward(0)
        sent, done = 1, 0
        for coarse in range(coarse_dev):
            low = 2 * coarse
            left = jnp.where(
                inner,
                jnp.where(odd, formed[low + 1], formed[low]),
                jnp.where(odd, ends[low + 1], ends[low]),
            )
            lefts.append(left)
            near = [(formed[low + step], ends[low + step], flag) for step in range(2)]
            out = correlate(out, left, near, left_scale, right_scale, coarse, coarse_dev, 2 * side, pols)
            if sent < len(steps):
                out, crossed[sent] = lax.optimization_barrier((out, crossed[sent]))
                forward(sent)
                sent += 1
        while done < len(steps):
            if sent < len(steps):
                out = far_part(out, done)
                done += 1
                out, crossed[sent] = lax.optimization_barrier((out, crossed[sent]))
                forward(sent)
                sent += 1
            else:
                out = far_part(out, done)
                done += 1
    out = out.reshape(2, coarse_dev, own_count, STATIONS, beams, pols, tiles, pols, LANES)
    out = jnp.swapaxes(out, -3, -2).reshape(2, coarse_dev, own_count, STATIONS, beams, pols, pols, fine)
    return out[None]


def solution(mesh):
    in_specs = (
        P(None, "chan", "stn", "tm", None, None),
        P(),
        P("stn"),
        P("stn"),
        P(None, None, "chan", None),
    )
    out_specs = P("tm", None, "chan", "stn", None, None, None, None, None)
    return jax.shard_map(
        per_device, mesh=mesh, in_specs=in_specs, out_specs=out_specs, check_vma=False
    )
```

```python
import jax
import jax.numpy as jnp
from jax import lax
from jax.experimental import pallas as pl
from jax.experimental.pallas import tpu as pltpu
from jax.sharding import PartitionSpec as P


STATIONS = 32
COARSE = 8
LANES = 128
UNROLL = 8
PARTS = 2
PREPARE = 4
PAIRS = (2, 4)

epsilon = 1e-06


def shifted(value, axis, steps):
    count = lax.axis_size(axis)
    first, last = (max(0, -steps), min(count, count - steps))
    return lax.ppermute(value, axis, [(source, source + steps) for source in range(first, last)])


def dft_tables(length):
    bin_index = jnp.arange(length, dtype=jnp.int32)
    phase_step = bin_index[:, None] * bin_index[None, :] % length
    angles = phase_step.astype(jnp.float32) * (2.0 * jnp.pi / length)
    return (jnp.cos(angles).astype(jnp.bfloat16), jnp.sin(angles).astype(jnp.bfloat16))


def block_ranks(station_map, block_stations, share):
    block = station_map // block_stations
    position = jnp.arange(station_map.shape[-1], dtype=jnp.int32)
    same = block[..., :, None] == block[..., None, :]
    before = position[None, :] < position[:, None]
    return block * share + jnp.sum((same & before).astype(jnp.int32), axis=-1)


def sort_dishes(voltages, order, coarse, parts, share):
    comps, _, _, frames, pols, fine = voltages.shape
    tiles = fine // LANES

    def body(order_ref, x_ref, *refs):
        outs, sems = refs[: len(parts)], refs[len(parts) :]

        def issue(place, carry):
            for part, out_ref, sem in zip(parts, outs, sems):
                dish = order_ref[part * share + place]
                for tile in range(tiles):
                    lanes = pl.ds(tile * LANES, LANES)
                    pltpu.make_async_copy(
                        x_ref.at[:, coarse, dish, :, :, lanes], out_ref.at[:, :, tile, place], sem
                    ).start()
            return carry

        lax.fori_loop(0, share, issue, 0)
        for out_ref, sem in zip(outs, sems):
            pltpu.make_async_copy(out_ref, out_ref, sem).wait()

    results = pl.pallas_call(
        body,
        out_shape=[jax.ShapeDtypeStruct((comps, frames, tiles, share, pols, LANES), voltages.dtype)] * len(parts),
        in_specs=[pl.BlockSpec(memory_space=pltpu.SMEM), pl.BlockSpec(memory_space=pl.ANY)],
        out_specs=[pl.BlockSpec(memory_space=pltpu.VMEM)] * len(parts),
        scratch_shapes=[pltpu.SemaphoreType.DMA] * len(parts),
        name="sort_dishes",
    )(order, voltages)

    return [array.reshape(comps, frames, tiles, share * pols, LANES) for array in results]


def beam_sums(weights, sources, frames_step=4):
    comps, frames, tiles, rows, _ = sources[0].shape
    out_rows, contract = weights.shape

    def body(w_ref, *refs):
        out_ref = refs[-1]
        for frame in range(frames_step):
            pieces = []
            for ref in refs[:-1]:
                for comp in range(comps):
                    pieces.append(jnp.concatenate([ref[comp, frame, t] for t in range(tiles)], axis=1))
            stacked = jnp.concatenate(pieces, axis=0)
            out_ref[frame] = jnp.dot(
                w_ref[...], stacked, preferred_element_type=jnp.float32
            ).astype(out_ref.dtype)

    return pl.pallas_call(
        body,
        grid=(frames // frames_step,),
        in_specs=[pl.BlockSpec((out_rows, contract), lambda i: (0, 0))]
        + [pl.BlockSpec((comps, frames_step, tiles, rows, LANES), lambda i: (0, i, 0, 0, 0))] * len(sources),
        out_specs=pl.BlockSpec((frames_step, out_rows, tiles * LANES), lambda i: (i, 0, 0)),
        out_shape=jax.ShapeDtypeStruct((frames, out_rows, tiles * LANES), jnp.bfloat16),
        name="beam_sums",
    )(weights, *sources)


def channelize(previous, current, taps, cosine, sine, beams):
    frames, out_rows, fine = current.shape
    taps_count = taps.shape[0]
    history = taps_count - 1
    rows = out_rows // (2 * beams)
    tiles = fine // LANES
    previous = previous.reshape(frames, 2, beams * rows, fine)
    current = current.reshape(frames, 2, beams * rows, fine)
    wide_taps = jnp.broadcast_to(taps[:, None, :], (taps_count, 8, fine))

    def body(prev_ref, cur_ref, taps_ref, cos_ref, sin_ref, out_ref, pow_ref, wide_ref, filt_ref):
        for frame in range(history):
            wide_ref[frame] = prev_ref[frames - history + frame].astype(jnp.float32)
        for frame in range(frames):
            wide_ref[history + frame] = cur_ref[frame].astype(jnp.float32)
        for comp in range(2):
            for tile in range(tiles):
                lanes = slice(tile * LANES, (tile + 1) * LANES)
                for low in range(0, rows, 8):
                    for frame in range(frames):
                        terms = [
                            taps_ref[tap, :, lanes]
                            * wide_ref[history + frame - tap, comp, low : low + 8, lanes]
                            for tap in range(taps_count)
                        ]
                        while len(terms) > 1:
                            terms = [
                                a + b for a, b in zip(terms[::2], terms[1::2])
                            ] + terms[len(terms) // 2 * 2 :]
                        filt_ref[comp, frame * rows + low : frame * rows + low + 8, lanes] = terms[0]
        real_part = filt_ref[0].astype(jnp.bfloat16)
        imag_part = filt_ref[1].astype(jnp.bfloat16)

        def dot(a, b):
            return jnp.dot(a, b, preferred_element_type=jnp.float32)

        spec_re = dot(real_part, cos_ref[...]) + dot(imag_part, sin_ref[...])
        spec_im = dot(imag_part, cos_ref[...]) - dot(real_part, sin_ref[...])
        power = jnp.zeros((rows, LANES), jnp.float32)
        for comp, spectrum in enumerate((spec_re, spec_im)):
            rounded = spectrum.astype(jnp.bfloat16)
            squares = rounded.astype(jnp.float32)
            squares = squares * squares
            for tile in range(tiles):
                lanes = slice(tile * LANES, (tile + 1) * LANES)
                for frame in range(frames):
                    out_ref[0, comp, frame, tile * rows : (tile + 1) * rows, :] = rounded[
                        frame * rows : (frame + 1) * rows, lanes
                    ]
                    power = power + squares[frame * rows : (frame + 1) * rows, lanes]
        pow_ref[0] = power

    return pl.pallas_call(
        body,
        grid=(beams,),
        in_specs=[
            pl.BlockSpec((frames, 2, rows, fine), lambda b: (0, 0, b, 0)),
            pl.BlockSpec((frames, 2, rows, fine), lambda b: (0, 0, b, 0)),
            pl.BlockSpec((taps_count, 8, fine), lambda b: (0, 0, 0)),
            pl.BlockSpec((fine, fine), lambda b: (0, 0)),
            pl.BlockSpec((fine, fine), lambda b: (0, 0)),
        ],
        out_specs=[
            pl.BlockSpec((1, 2, frames, tiles * rows, LANES), lambda b: (b, 0, 0, 0, 0)),
            pl.BlockSpec((1, rows, LANES), lambda b: (b, 0, 0)),
        ],
        out_shape=[
            jax.ShapeDtypeStruct((beams, 2, frames, tiles * rows, LANES), jnp.bfloat16),
            jax.ShapeDtypeStruct((beams, rows, LANES), jnp.float32),
        ],
        scratch_shapes=[
            pltpu.VMEM((history + frames, 2, rows, fine), jnp.float32),
            pltpu.VMEM((2, frames * rows, fine), jnp.float32),
        ],
        name="channelize",
    )(previous, current, wide_taps, cosine, sine)


def spread_matrix(stations, pols, tiles, left):
    shape = (stations, pols, tiles, pols)
    station, p, tile, q = (lax.broadcasted_iota(jnp.int32, shape, axis).reshape(-1) for axis in range(4))
    source = (tile * stations + station) * pols + (p if left else q)
    column = jnp.arange(tiles * stations * pols, dtype=jnp.int32)
    return (source[:, None] == column[None, :]).astype(jnp.bfloat16)


def correlate(out, left, rights, left_scale, right_scale, coarse, coarse_count, block, pols, low_beam=0):
    some_beams, _, frames, rows, _ = left.shape
    beams, own, unit, _ = left_scale.shape
    stations = right_scale.shape[1]
    tiles = unit // (pols * pols)
    blocks = len(rights)
    others = own * blocks
    size = own * unit
    spread_left = spread_matrix(own, pols, tiles, True)
    spread_right = spread_matrix(own, pols, tiles, False)
    pair_left, pair_right = PAIRS
    choice = [right if isinstance(right, tuple) else (right,) for right in rights]
    flag = next((right[2] for right in choice if len(right) == 3), 0)
    arrays = [array for right in choice for array in right[:2]]
    scalars = jnp.stack([jnp.asarray(block, jnp.int32), jnp.asarray(flag, jnp.int32)])

    def body(scalar_ref, *refs):
        left_ref, sl_ref, pl_ref, pr_ref = refs[:4]
        right_refs = list(refs[4 : 4 + len(arrays)])
        sr_ref = refs[4 + len(arrays)]
        out_ref, l_ref, r_ref = refs[-3:]

        def spread(matrix_ref, pieces, scale):
            wide = jnp.dot(
                matrix_ref[...], jnp.concatenate(pieces, axis=1), preferred_element_type=jnp.float32
            )
            return [wide[:, i * LANES : (i + 1) * LANES] * scale for i in range(len(pieces))]

        def chosen(index, frame):
            place = sum(min(len(c), 2) for c in choice[:index])
            halves = [right_refs[place][0, o, frame] for o in range(2)]
            if len(choice[index]) == 3:
                second = right_refs[place + 1]
                halves = [jnp.where(scalar_ref[1] == 0, halves[o], second[0, o, frame]) for o in range(2)]
            return halves

        span = PREPARE
        left_scales = sl_ref[0].reshape(size, LANES)
        for first in range(0, frames, span):
            those = range(first, first + span)
            parts = spread(pl_ref, [left_ref[0, o, f] for f in those for o in range(2)], left_scales)
            for frame in those:
                real, imag = parts[2 * (frame - first)], parts[2 * (frame - first) + 1]
                l_ref[frame, 0] = real
                l_ref[frame, 1] = imag
                l_ref[frame, 2] = real + imag
        for index in range(blocks):
            low, high = index * size, (index + 1) * size
            scale = sr_ref[0, index * own : (index + 1) * own].reshape(size, LANES)
            for first in range(0, frames, span):
                those = range(first, first + span)
                parts = spread(pr_ref, [half for f in those for half in chosen(index, f)], scale)
                for frame in those:
                    real, imag = parts[2 * (frame - first)], parts[2 * (frame - first) + 1]
                    r_ref[frame, 0, low:high] = real
                    r_ref[frame, 1, low:high] = imag
                    r_ref[frame, 2, low:high] = real - imag

        left_groups = own // pair_left

        def products(step, carry):
            first_left = (step % left_groups) * pair_left
            first_right = (step // left_groups) * pair_right
            pairs = [(i, j) for i in range(pair_left) for j in range(pair_right)]

            def add_frame(frame, sums):
                lefts = [
                    [l_ref[frame, k, pl.ds((first_left + i) * unit, unit)] for k in range(3)]
                    for i in range(pair_left)
                ]
                result = []
                for j in range(pair_right):
                    right = [r_ref[frame, k, pl.ds((first_right + j) * unit, unit)] for k in range(3)]
                    for i in range(pair_left):
                        for k in range(3):
                            result.append(sums[(j * pair_left + i) * 3 + k] + lefts[i][k] * right[k])
                return tuple(result)

            zeros = tuple(jnp.zeros((unit, LANES), jnp.float32) for _ in range(3 * len(pairs)))
            sums = lax.fori_loop(0, frames, add_frame, zeros, unroll=UNROLL)
            for i, j in pairs:
                rr, ii, mixed = sums[(j * pair_left + i) * 3 : (j * pair_left + i) * 3 + 3]
                out_ref[0, 0, first_left + i, first_right + j, 0] = rr + ii
                out_ref[1, 0, first_left + i, first_right + j, 0] = mixed - rr + ii
            return carry

        lax.fori_loop(0, left_groups * (others // pair_right), products, 0)

    beam_spec = pl.BlockSpec((1, 2, frames, rows, LANES), lambda b, s: (b, 0, 0, 0, 0))
    operands = [left, left_scale, spread_left, spread_right, *arrays, right_scale]
    in_specs = [
        beam_spec,
        pl.BlockSpec((1, own, unit, LANES), lambda b, s: (low_beam + b, 0, 0, 0)),
        pl.BlockSpec(spread_left.shape, lambda b, s: (0, 0)),
        pl.BlockSpec(spread_right.shape, lambda b, s: (0, 0)),
        *[beam_spec for _ in arrays],
        pl.BlockSpec((1, others, unit, LANES), lambda b, s: (low_beam + b, s[0] // blocks, 0, 0)),
    ]
    aliases = {}
    if out is not None:
        aliases = {1 + len(operands): 0}
        operands.append(out)
        in_specs.append(pl.BlockSpec(memory_space=pl.ANY))
    shape = (2, coarse_count, own, stations, beams, unit, LANES)
    return pl.pallas_call(
        body,
        grid_spec=pltpu.PrefetchScalarGridSpec(
            num_scalar_prefetch=1,
            grid=(some_beams,),
            in_specs=in_specs,
            out_specs=pl.BlockSpec(
                (2, 1, own, others, 1, unit, LANES),
                lambda b, s: (0, coarse, 0, s[0] // blocks, low_beam + b, 0, 0),
            ),
            scratch_shapes=[
                pltpu.VMEM((frames, 3, size, LANES), jnp.float32),
                pltpu.VMEM((frames, 3, others * unit, LANES), jnp.float32),
            ],
        ),
        out_shape=jax.ShapeDtypeStruct(shape, jnp.float32),
        input_output_aliases=aliases,
    )(scalars, *operands)


def block_weights(maps, weight_table, target, block_stations, share, pols):
    stations, rows = maps[:, 0], maps[:, 1]
    groups = maps.shape[0]
    _, table_rows, coarse, beams = weight_table.shape
    ranks = block_ranks(stations, block_stations, share)
    place = target * share + jnp.arange(share, dtype=jnp.int32)
    chosen = ranks[:, None, :] == place[None, :, None]
    station = jnp.sum(jnp.where(chosen, stations[:, None, :], 0), axis=-1) - target * block_stations
    row = jnp.sum(jnp.where(chosen, rows[:, None, :], 0), axis=-1)
    columns = (groups, 2, share, pols)
    out_rows = (2, beams, block_stations, pols)
    station = jnp.broadcast_to(station[:, None, :, None], columns).reshape(1, -1)
    row = jnp.broadcast_to(row[:, None, :, None], columns).reshape(1, -1)
    part, pol = (lax.broadcasted_iota(jnp.int32, columns, axis).reshape(1, -1) for axis in (1, 3))
    own_station, own_pol = (lax.broadcasted_iota(jnp.int32, out_rows, axis).reshape(-1, 1) for axis in (2, 3))
    term = jnp.arange(2 * table_rows, dtype=jnp.int32)[:, None]
    hot = (term == part * table_rows + row).astype(jnp.bfloat16)
    kept = (station == own_station) & (pol == own_pol)
    real, imag = weight_table[0], weight_table[1]
    mixing = jnp.stack([jnp.concatenate([real, -imag]), jnp.concatenate([imag, real])])
    result = []
    for channel in range(coarse):
        table = mixing[:, :, channel].swapaxes(1, 2)[:, :, None, None]
        table = jnp.broadcast_to(table, out_rows + (2 * table_rows,)).reshape(-1, 2 * table_rows)
        values = jnp.dot(table, hot, preferred_element_type=jnp.float32)
        result.append(jnp.where(kept, values, 0.0).astype(jnp.bfloat16))
    return result


def scales(power, denominator, frames, own_index, tiles):
    inverse = lax.rsqrt(power / denominator + epsilon)
    blocks, beams, own_count, pols = inverse.shape
    inverse = jnp.moveaxis(inverse, 1, 0).reshape(beams, blocks * own_count, pols)
    full = (beams, blocks * own_count, pols, tiles, pols, LANES)
    unit = pols * tiles * pols
    right = jnp.broadcast_to(inverse[:, :, None, None, :, None] / frames, full)
    mine = lax.dynamic_slice_in_dim(inverse, own_index * own_count, own_count, 1)
    left = jnp.broadcast_to(mine[:, :, :, None, None, None], (beams, own_count) + full[2:])
    return left.reshape(beams, own_count, unit, LANES), right.reshape(beams, blocks * own_count, unit, LANES)


def per_device(voltages, fir_taps, station_map, beam_index, weight_table):
    _, coarse_dev, dishes_dev, frames, pols, fine = voltages.shape
    groups = lax.axis_size("stn")
    own_index = lax.axis_index("stn")
    beams = weight_table.shape[3]
    share = dishes_dev // groups
    own_count = STATIONS // groups
    tiles = fine // LANES
    denominator = COARSE * frames * fine
    cosine, sine = dft_tables(fine)
    places = jnp.arange(dishes_dev, dtype=jnp.int32)
    line = groups == 4
    side = own_index // 2 if line else 0
    ranks = block_ranks(station_map, own_count, share)
    ranks = (ranks + 2 * side * share) % dishes_dev
    order = jnp.sum(jnp.where(ranks[None, :] == places[:, None], places[None, :], 0), axis=1)
    maps = jnp.stack([station_map, beam_index])

    def form(weights, sources, beams):
        sums = beam_sums(weights, sources)
        earlier = shifted(sums, "tm", 1)
        formed, lane_power = channelize(earlier, sums, fir_taps, cosine, sine, beams)
        return formed, jnp.sum(lane_power, axis=-1)

    def place_power(power):
        return power.reshape(groups, beams, own_count, pols)

    out = None
    if not line:
        maps = lax.all_gather(maps, "stn")
        weights = block_weights(maps, weight_table, own_index, own_count, share, pols)
        formed, power = [], 0.0
        for coarse in range(coarse_dev):
            blocks = jnp.stack(sort_dishes(voltages, order, coarse, range(groups), share))
            arrived = lax.all_to_all(blocks, "stn", 0, 0, tiled=True)
            own, more = form(weights[coarse], [arrived[g] for g in range(groups)], beams)
            power = power + more
            formed.append((own, lax.all_gather(own, "stn")))
        power = place_power(lax.psum(lax.all_gather(power, "stn"), "chan"))
        left_scale, right_scale = scales(power, denominator, frames, own_index, tiles)
        for coarse in range(coarse_dev):
            own, everyone = formed[coarse]
            rights = [everyone[g] for g in range(groups)]
            out = correlate(out, own, rights, left_scale, right_scale, coarse, coarse_dev, 0, pols)
    else:
        inward, across, outward = [(0, 1), (3, 2)], [(1, 2), (2, 1)], [(1, 0), (2, 3)]
        beyond_one = [(0, 2), (3, 1)]
        inner = (own_index == 1) | (own_index == 2)
        paths = (inward, across, beyond_one)
        known = [maps]
        for path in paths:
            known.append(lax.ppermute(maps, "stn", path))
        maps = jnp.stack(known)
        some = beams // PARTS
        weights = [
            [
                block_weights(
                    maps, weight_table[..., part * some : (part + 1) * some], 2 * side + step, own_count, share, pols
                )
                for part in range(PARTS)
            ]
            for step in range(2)
        ]
        steps = [(coarse, step) for coarse in range(coarse_dev) for step in range(2)]
        arrived = []
        for coarse, step in steps:
            index = len(arrived)
            near, far = sort_dishes(voltages, order, coarse, (step, 2 + step), share)
            sources = [near]
            for sent, path in zip((near, far, far), paths):
                sources.append(lax.ppermute(sent, "stn", path))
            arrived.append(sources)
        formed, ends, power = {}, {}, [[0.0] * PARTS for _ in range(2)]
        keys = [(*key, part) for key in steps for part in range(PARTS)]
        crossed = {}
        for index, (coarse, step, part) in enumerate(keys):
            sources = arrived[index // PARTS]
            if index:
                _, sources = lax.optimization_barrier((formed[keys[index - 1]], sources))
            own, more = form(weights[step][part][coarse], sources, some)
            formed[coarse, step, part] = own
            power[step][part] = power[step][part] + more
            ends[coarse, step, part] = lax.ppermute(own, "stn", outward)
            if index < PARTS:
                crossed[coarse, step, part] = lax.ppermute(own, "stn", across)
        power = jnp.stack([jnp.concatenate(parts) for parts in power])
        power = lax.psum(power, "chan")
        beyond = lax.ppermute(power, "stn", across)
        beyond, *held = lax.optimization_barrier((beyond, *[formed[key] for key in keys[PARTS:]]))
        for index, value in enumerate(held, PARTS):
            crossed[keys[index]] = lax.ppermute(value, "stn", across)
        both = jnp.stack([power, beyond])
        from_inner = lax.ppermute(both, "stn", outward)
        flag = jnp.where(inner, 0, 1)
        odd = own_index % 2 == 1
        held = [crossed[key] for key in keys[:PARTS]] + [ends[key] for key in keys]
        from_inner, *held = lax.optimization_barrier((from_inner, *held))
        crossed.update(zip(keys[:PARTS], held))
        ends = dict(zip(keys, held[PARTS:]))
        both = jnp.where(inner, both, from_inner)
        power = jnp.where(side == 0, both, both[::-1]).reshape((groups,) + power.shape[1:])
        left_scale, right_scale = scales(place_power(power), denominator, frames, own_index, tiles)
        far_ends, lefts = {}, {}

        def forward(index):
            far_ends[keys[index]] = lax.ppermute(crossed[keys[index]], "stn", outward)

        def near_work(out, coarse, part):
            lefts[coarse, part] = jnp.where(
                inner,
                jnp.where(odd, formed[coarse, 1, part], formed[coarse, 0, part]),
                jnp.where(odd, ends[coarse, 1, part], ends[coarse, 0, part]),
            )
            near = [(formed[coarse, step, part], ends[coarse, step, part], flag) for step in range(2)]
            return correlate(
                out, lefts[coarse, part], near, left_scale, right_scale, coarse, coarse_dev,
                2 * side, pols, part * some,
            )

        def far_work(out, coarse, step, part):
            far = [(crossed[coarse, step, part], far_ends[coarse, step, part], flag)]
            return correlate(
                out, lefts[coarse, part], far, left_scale, right_scale, coarse, coarse_dev,
                2 * (1 - side) + step, pols, part * some,
            )

        work = [(near_work, (coarse, part)) for coarse in range(coarse_dev) for part in range(PARTS)]
        work += [(far_work, key) for key in keys]
        for index in range(PARTS):
            forward(index)
        for index, (make, which) in enumerate(work):
            out = make(out, *which)
            sent = index + PARTS
            if sent < len(keys):
                out, crossed[keys[sent]] = lax.optimization_barrier((out, crossed[keys[sent]]))
                forward(sent)
    out = out.reshape(2, coarse_dev, own_count, STATIONS, beams, pols, tiles, pols, LANES)
    out = jnp.swapaxes(out, -3, -2).reshape(2, coarse_dev, own_count, STATIONS, beams, pols, pols, fine)
    return out[None]


def solution(mesh):
    in_specs = (
        P(None, "chan", "stn", "tm", None, None),
        P(),
        P("stn"),
        P("stn"),
        P(None, None, "chan", None),
    )
    out_specs = P("tm", None, "chan", "stn", None, None, None, None, None)
    return jax.shard_map(
        per_device, mesh=mesh, in_specs=in_specs, out_specs=out_specs, check_vma=False
    )
```

```python
import jax
import jax.numpy as jnp
from jax import lax
from jax.experimental import pallas as pl
from jax.experimental.pallas import tpu as pltpu
from jax.sharding import PartitionSpec as P


STATIONS = 32
COARSE = 8
LANES = 128
UNROLL = 8
PREPARE = 4
PAIRS = (2, 4)

epsilon = 1e-06


def shifted(value, axis, steps):
    count = lax.axis_size(axis)
    first, last = (max(0, -steps), min(count, count - steps))
    return lax.ppermute(value, axis, [(source, source + steps) for source in range(first, last)])


def dft_tables(length):
    bin_index = jnp.arange(length, dtype=jnp.int32)
    phase_step = bin_index[:, None] * bin_index[None, :] % length
    angles = phase_step.astype(jnp.float32) * (2.0 * jnp.pi / length)
    return (jnp.cos(angles).astype(jnp.bfloat16), jnp.sin(angles).astype(jnp.bfloat16))


def block_ranks(station_map, block_stations, share):
    block = station_map // block_stations
    position = jnp.arange(station_map.shape[-1], dtype=jnp.int32)
    same = block[..., :, None] == block[..., None, :]
    before = position[None, :] < position[:, None]
    return block * share + jnp.sum((same & before).astype(jnp.int32), axis=-1)


def sort_dishes(voltages, order, coarse, parts, share):
    comps, _, _, frames, pols, fine = voltages.shape
    tiles = fine // LANES

    def body(order_ref, x_ref, *refs):
        outs, sems = refs[: len(parts)], refs[len(parts) :]

        def issue(place, carry):
            for part, out_ref, sem in zip(parts, outs, sems):
                dish = order_ref[part * share + place]
                for tile in range(tiles):
                    lanes = pl.ds(tile * LANES, LANES)
                    pltpu.make_async_copy(
                        x_ref.at[:, coarse, dish, :, :, lanes], out_ref.at[:, :, tile, place], sem
                    ).start()
            return carry

        lax.fori_loop(0, share, issue, 0)
        for out_ref, sem in zip(outs, sems):
            pltpu.make_async_copy(out_ref, out_ref, sem).wait()

    results = pl.pallas_call(
        body,
        out_shape=[jax.ShapeDtypeStruct((comps, frames, tiles, share, pols, LANES), voltages.dtype)] * len(parts),
        in_specs=[pl.BlockSpec(memory_space=pltpu.SMEM), pl.BlockSpec(memory_space=pl.ANY)],
        out_specs=[pl.BlockSpec(memory_space=pltpu.VMEM)] * len(parts),
        scratch_shapes=[pltpu.SemaphoreType.DMA] * len(parts),
        name="sort_dishes",
    )(order, voltages)

    return [array.reshape(comps, frames, tiles, share * pols, LANES) for array in results]


def beam_sums(weights, sources, frames_step=4):
    comps, frames, tiles, rows, _ = sources[0].shape
    out_rows, contract = weights.shape

    def body(w_ref, *refs):
        out_ref = refs[-1]
        for frame in range(frames_step):
            pieces = []
            for ref in refs[:-1]:
                for comp in range(comps):
                    pieces.append(jnp.concatenate([ref[comp, frame, t] for t in range(tiles)], axis=1))
            stacked = jnp.concatenate(pieces, axis=0)
            out_ref[frame] = jnp.dot(
                w_ref[...], stacked, preferred_element_type=jnp.float32
            ).astype(out_ref.dtype)

    return pl.pallas_call(
        body,
        grid=(frames // frames_step,),
        in_specs=[pl.BlockSpec((out_rows, contract), lambda i: (0, 0))]
        + [pl.BlockSpec((comps, frames_step, tiles, rows, LANES), lambda i: (0, i, 0, 0, 0))] * len(sources),
        out_specs=pl.BlockSpec((frames_step, out_rows, tiles * LANES), lambda i: (i, 0, 0)),
        out_shape=jax.ShapeDtypeStruct((frames, out_rows, tiles * LANES), jnp.bfloat16),
        name="beam_sums",
    )(weights, *sources)


def channelize(previous, current, taps, cosine, sine, beams):
    frames, out_rows, fine = current.shape
    taps_count = taps.shape[0]
    history = taps_count - 1
    rows = out_rows // (2 * beams)
    tiles = fine // LANES
    previous = previous.reshape(frames, 2, beams * rows, fine)
    current = current.reshape(frames, 2, beams * rows, fine)
    wide_taps = jnp.broadcast_to(taps[:, None, :], (taps_count, 8, fine))

    def body(prev_ref, cur_ref, taps_ref, cos_ref, sin_ref, out_ref, pow_ref, wide_ref, filt_ref):
        for frame in range(history):
            wide_ref[frame] = prev_ref[frames - history + frame].astype(jnp.float32)
        for frame in range(frames):
            wide_ref[history + frame] = cur_ref[frame].astype(jnp.float32)
        groups = rows // 8

        def filter_rows(index, carry):
            comp = index // groups
            low = pl.multiple_of(index % groups * 8, 8)
            for tile in range(tiles):
                lanes = slice(tile * LANES, (tile + 1) * LANES)
                for frame in range(frames):
                    terms = [
                        taps_ref[tap, :, lanes] * wide_ref[history + frame - tap, comp, pl.ds(low, 8), lanes]
                        for tap in range(taps_count)
                    ]
                    while len(terms) > 1:
                        odd = terms[len(terms) // 2 * 2 :]
                        terms = [a + b for a, b in zip(terms[::2], terms[1::2])] + odd
                    filt_ref[comp, pl.ds(frame * rows + low, 8), lanes] = terms[0]
            return carry

        lax.fori_loop(0, 2 * groups, filter_rows, 0)
        real_part = filt_ref[0].astype(jnp.bfloat16)
        imag_part = filt_ref[1].astype(jnp.bfloat16)

        def dot(a, b):
            return jnp.dot(a, b, preferred_element_type=jnp.float32)

        spec_re = dot(real_part, cos_ref[...]) + dot(imag_part, sin_ref[...])
        spec_im = dot(imag_part, cos_ref[...]) - dot(real_part, sin_ref[...])
        power = jnp.zeros((rows, LANES), jnp.float32)
        for comp, spectrum in enumerate((spec_re, spec_im)):
            rounded = spectrum.astype(jnp.bfloat16)
            squares = rounded.astype(jnp.float32)
            squares = squares * squares
            for tile in range(tiles):
                lanes = slice(tile * LANES, (tile + 1) * LANES)
                for frame in range(frames):
                    out_ref[0, comp, frame, tile * rows : (tile + 1) * rows, :] = rounded[
                        frame * rows : (frame + 1) * rows, lanes
                    ]
                    power = power + squares[frame * rows : (frame + 1) * rows, lanes]
        pow_ref[0] = power

    return pl.pallas_call(
        body,
        grid=(beams,),
        in_specs=[
            pl.BlockSpec((frames, 2, rows, fine), lambda b: (0, 0, b, 0)),
            pl.BlockSpec((frames, 2, rows, fine), lambda b: (0, 0, b, 0)),
            pl.BlockSpec((taps_count, 8, fine), lambda b: (0, 0, 0)),
            pl.BlockSpec((fine, fine), lambda b: (0, 0)),
            pl.BlockSpec((fine, fine), lambda b: (0, 0)),
        ],
        out_specs=[
            pl.BlockSpec((1, 2, frames, tiles * rows, LANES), lambda b: (b, 0, 0, 0, 0)),
            pl.BlockSpec((1, rows, LANES), lambda b: (b, 0, 0)),
        ],
        out_shape=[
            jax.ShapeDtypeStruct((beams, 2, frames, tiles * rows, LANES), jnp.bfloat16),
            jax.ShapeDtypeStruct((beams, rows, LANES), jnp.float32),
        ],
        scratch_shapes=[
            pltpu.VMEM((history + frames, 2, rows, fine), jnp.float32),
            pltpu.VMEM((2, frames * rows, fine), jnp.float32),
        ],
        name="channelize",
    )(previous, current, wide_taps, cosine, sine)


def spread_matrix(stations, pols, tiles, left):
    shape = (stations, pols, tiles, pols)
    station, p, tile, q = (lax.broadcasted_iota(jnp.int32, shape, axis).reshape(-1) for axis in range(4))
    source = (tile * stations + station) * pols + (p if left else q)
    column = jnp.arange(tiles * stations * pols, dtype=jnp.int32)
    return (source[:, None] == column[None, :]).astype(jnp.bfloat16)


def correlate(out, left, rights, left_scale, right_scale, coarse, coarse_count, block, pols, low_beam=0):
    some_beams, _, frames, rows, _ = left.shape
    beams, own, unit, _ = left_scale.shape
    stations = right_scale.shape[1]
    tiles = unit // (pols * pols)
    blocks = len(rights)
    others = own * blocks
    size = own * unit
    spread_left = spread_matrix(own, pols, tiles, True)
    spread_right = spread_matrix(own, pols, tiles, False)
    pair_left, pair_right = PAIRS
    choice = [right if isinstance(right, tuple) else (right,) for right in rights]
    flag = next((right[2] for right in choice if len(right) == 3), 0)
    arrays = [array for right in choice for array in right[:2]]
    scalars = jnp.stack([jnp.asarray(block, jnp.int32), jnp.asarray(flag, jnp.int32)])

    def body(scalar_ref, *refs):
        left_ref, sl_ref, pl_ref, pr_ref = refs[:4]
        right_refs = list(refs[4 : 4 + len(arrays)])
        sr_ref = refs[4 + len(arrays)]
        out_ref, l_ref, r_ref = refs[-3:]

        def spread(matrix_ref, pieces, scale):
            wide = jnp.dot(
                matrix_ref[...], jnp.concatenate(pieces, axis=1), preferred_element_type=jnp.float32
            )
            return [wide[:, i * LANES : (i + 1) * LANES] * scale for i in range(len(pieces))]

        def chosen(index, frame):
            place = sum(min(len(c), 2) for c in choice[:index])
            halves = [right_refs[place][0, o, frame] for o in range(2)]
            if len(choice[index]) == 3:
                second = right_refs[place + 1]
                halves = [jnp.where(scalar_ref[1] == 0, halves[o], second[0, o, frame]) for o in range(2)]
            return halves

        span = PREPARE
        left_scales = sl_ref[0].reshape(size, LANES)
        for first in range(0, frames, span):
            those = range(first, first + span)
            parts = spread(pl_ref, [left_ref[0, o, f] for f in those for o in range(2)], left_scales)
            for frame in those:
                real, imag = parts[2 * (frame - first)], parts[2 * (frame - first) + 1]
                l_ref[frame, 0] = real
                l_ref[frame, 1] = imag
                l_ref[frame, 2] = real + imag
        for index in range(blocks):
            low, high = index * size, (index + 1) * size
            scale = sr_ref[0, index * own : (index + 1) * own].reshape(size, LANES)
            for first in range(0, frames, span):
                those = range(first, first + span)
                parts = spread(pr_ref, [half for f in those for half in chosen(index, f)], scale)
                for frame in those:
                    real, imag = parts[2 * (frame - first)], parts[2 * (frame - first) + 1]
                    r_ref[frame, 0, low:high] = real
                    r_ref[frame, 1, low:high] = imag
                    r_ref[frame, 2, low:high] = real - imag

        left_groups = own // pair_left

        def products(step, carry):
            first_left = (step % left_groups) * pair_left
            first_right = (step // left_groups) * pair_right
            pairs = [(i, j) for i in range(pair_left) for j in range(pair_right)]

            def add_frame(frame, sums):
                lefts = [
                    [l_ref[frame, k, pl.ds((first_left + i) * unit, unit)] for k in range(3)]
                    for i in range(pair_left)
                ]
                result = []
                for j in range(pair_right):
                    right = [r_ref[frame, k, pl.ds((first_right + j) * unit, unit)] for k in range(3)]
                    for i in range(pair_left):
                        for k in range(3):
                            result.append(sums[(j * pair_left + i) * 3 + k] + lefts[i][k] * right[k])
                return tuple(result)

            zeros = tuple(jnp.zeros((unit, LANES), jnp.float32) for _ in range(3 * len(pairs)))
            sums = lax.fori_loop(0, frames, add_frame, zeros, unroll=UNROLL)
            for i, j in pairs:
                rr, ii, mixed = sums[(j * pair_left + i) * 3 : (j * pair_left + i) * 3 + 3]
                out_ref[0, 0, first_left + i, first_right + j, 0] = rr + ii
                out_ref[1, 0, first_left + i, first_right + j, 0] = mixed - rr + ii
            return carry

        lax.fori_loop(0, left_groups * (others // pair_right), products, 0)

    beam_spec = pl.BlockSpec((1, 2, frames, rows, LANES), lambda b, s: (b, 0, 0, 0, 0))
    operands = [left, left_scale, spread_left, spread_right, *arrays, right_scale]
    in_specs = [
        beam_spec,
        pl.BlockSpec((1, own, unit, LANES), lambda b, s: (low_beam + b, 0, 0, 0)),
        pl.BlockSpec(spread_left.shape, lambda b, s: (0, 0)),
        pl.BlockSpec(spread_right.shape, lambda b, s: (0, 0)),
        *[beam_spec for _ in arrays],
        pl.BlockSpec((1, others, unit, LANES), lambda b, s: (low_beam + b, s[0] // blocks, 0, 0)),
    ]
    aliases = {}
    if out is not None:
        aliases = {1 + len(operands): 0}
        operands.append(out)
        in_specs.append(pl.BlockSpec(memory_space=pl.ANY))
    shape = (2, coarse_count, own, stations, beams, unit, LANES)
    return pl.pallas_call(
        body,
        grid_spec=pltpu.PrefetchScalarGridSpec(
            num_scalar_prefetch=1,
            grid=(some_beams,),
            in_specs=in_specs,
            out_specs=pl.BlockSpec(
                (2, 1, own, others, 1, unit, LANES),
                lambda b, s: (0, coarse, 0, s[0] // blocks, low_beam + b, 0, 0),
            ),
            scratch_shapes=[
                pltpu.VMEM((frames, 3, size, LANES), jnp.float32),
                pltpu.VMEM((frames, 3, others * unit, LANES), jnp.float32),
            ],
        ),
        out_shape=jax.ShapeDtypeStruct(shape, jnp.float32),
        input_output_aliases=aliases,
    )(scalars, *operands)


def block_weights(maps, weight_table, target, block_stations, share, pols):
    stations, rows = maps[:, 0], maps[:, 1]
    groups = maps.shape[0]
    _, table_rows, coarse, beams = weight_table.shape
    ranks = block_ranks(stations, block_stations, share)
    place = target * share + jnp.arange(share, dtype=jnp.int32)
    chosen = ranks[:, None, :] == place[None, :, None]
    station = jnp.sum(jnp.where(chosen, stations[:, None, :], 0), axis=-1) - target * block_stations
    row = jnp.sum(jnp.where(chosen, rows[:, None, :], 0), axis=-1)
    columns = (groups, 2, share, pols)
    out_rows = (2, beams, block_stations, pols)
    station = jnp.broadcast_to(station[:, None, :, None], columns).reshape(1, -1)
    row = jnp.broadcast_to(row[:, None, :, None], columns).reshape(1, -1)
    part, pol = (lax.broadcasted_iota(jnp.int32, columns, axis).reshape(1, -1) for axis in (1, 3))
    own_station, own_pol = (lax.broadcasted_iota(jnp.int32, out_rows, axis).reshape(-1, 1) for axis in (2, 3))
    term = jnp.arange(2 * table_rows, dtype=jnp.int32)[:, None]
    hot = (term == part * table_rows + row).astype(jnp.bfloat16)
    kept = (station == own_station) & (pol == own_pol)
    real, imag = weight_table[0], weight_table[1]
    mixing = jnp.stack([jnp.concatenate([real, -imag]), jnp.concatenate([imag, real])])
    result = []
    for channel in range(coarse):
        table = mixing[:, :, channel].swapaxes(1, 2)[:, :, None, None]
        table = jnp.broadcast_to(table, out_rows + (2 * table_rows,)).reshape(-1, 2 * table_rows)
        values = jnp.dot(table, hot, preferred_element_type=jnp.float32)
        result.append(jnp.where(kept, values, 0.0).astype(jnp.bfloat16))
    return result


def scales(power, denominator, frames, own_index, tiles):
    inverse = lax.rsqrt(power / denominator + epsilon)
    blocks, beams, own_count, pols = inverse.shape
    inverse = jnp.moveaxis(inverse, 1, 0).reshape(beams, blocks * own_count, pols)
    full = (beams, blocks * own_count, pols, tiles, pols, LANES)
    unit = pols * tiles * pols
    right = jnp.broadcast_to(inverse[:, :, None, None, :, None] / frames, full)
    mine = lax.dynamic_slice_in_dim(inverse, own_index * own_count, own_count, 1)
    left = jnp.broadcast_to(mine[:, :, :, None, None, None], (beams, own_count) + full[2:])
    return left.reshape(beams, own_count, unit, LANES), right.reshape(beams, blocks * own_count, unit, LANES)


def beam_parts(beams, last):
    half = beams // 2
    if not last:
        return [(0, half), (half, half)]
    return [(0, half), (half, half // 2), (half + half // 2, half - half // 2)]


def per_device(voltages, fir_taps, station_map, beam_index, weight_table):
    _, coarse_dev, dishes_dev, frames, pols, fine = voltages.shape
    groups = lax.axis_size("stn")
    own_index = lax.axis_index("stn")
    beams = weight_table.shape[3]
    share = dishes_dev // groups
    own_count = STATIONS // groups
    tiles = fine // LANES
    denominator = COARSE * frames * fine
    cosine, sine = dft_tables(fine)
    places = jnp.arange(dishes_dev, dtype=jnp.int32)
    line = groups == 4
    side = own_index // 2 if line else 0
    ranks = block_ranks(station_map, own_count, share)
    ranks = (ranks + 2 * side * share) % dishes_dev
    order = jnp.sum(jnp.where(ranks[None, :] == places[:, None], places[None, :], 0), axis=1)
    maps = jnp.stack([station_map, beam_index])

    def form(weights, sources, beams):
        sums = beam_sums(weights, sources)
        earlier = shifted(sums, "tm", 1)
        formed, lane_power = channelize(earlier, sums, fir_taps, cosine, sine, beams)
        return formed, jnp.sum(lane_power, axis=-1)

    def place_power(power):
        return power.reshape(groups, beams, own_count, pols)

    out = None
    if not line:
        maps = lax.all_gather(maps, "stn")
        weights = block_weights(maps, weight_table, own_index, own_count, share, pols)
        formed, power = [], 0.0
        for coarse in range(coarse_dev):
            blocks = jnp.stack(sort_dishes(voltages, order, coarse, range(groups), share))
            arrived = lax.all_to_all(blocks, "stn", 0, 0, tiled=True)
            own, more = form(weights[coarse], [arrived[g] for g in range(groups)], beams)
            power = power + more
            formed.append((own, lax.all_gather(own, "stn")))
        power = place_power(lax.psum(lax.all_gather(power, "stn"), "chan"))
        left_scale, right_scale = scales(power, denominator, frames, own_index, tiles)
        for coarse in range(coarse_dev):
            own, everyone = formed[coarse]
            rights = [everyone[g] for g in range(groups)]
            out = correlate(out, own, rights, left_scale, right_scale, coarse, coarse_dev, 0, pols)
    else:
        inward, across, outward = [(0, 1), (3, 2)], [(1, 2), (2, 1)], [(1, 0), (2, 3)]
        beyond_one = [(0, 2), (3, 1)]
        inner = (own_index == 1) | (own_index == 2)
        paths = (inward, across, beyond_one)
        known = [maps]
        for path in paths:
            known.append(lax.ppermute(maps, "stn", path))
        maps = jnp.stack(known)
        parts = [beam_parts(beams, coarse == coarse_dev - 1) for coarse in range(coarse_dev)]
        steps = [(coarse, step) for coarse in range(coarse_dev) for step in range(2)]
        arrived = []
        for coarse, step in steps:
            index = len(arrived)
            near, far = sort_dishes(voltages, order, coarse, (step, 2 + step), share)
            sources = [near]
            for sent, path in zip((near, far, far), paths):
                sources.append(lax.ppermute(sent, "stn", path))
            arrived.append(sources)
        formed, ends, powers = {}, {}, {}
        keys = [(coarse, step, part) for coarse, step in steps for part in parts[coarse]]
        early = len(parts[0])
        weights = {}
        for step in range(2):
            for part in {part: None for some in parts for part in some}:
                table = weight_table[..., part[0] : sum(part)]
                weights[step, part] = block_weights(maps, table, 2 * side + step, own_count, share, pols)
        crossed = {}
        for index, (coarse, step, part) in enumerate(keys):
            sources = arrived[steps.index((coarse, step))]
            if index:
                _, sources = lax.optimization_barrier((formed[keys[index - 1]], sources))
            own, powers[coarse, step, part] = form(weights[step, part][coarse], sources, part[1])
            formed[coarse, step, part] = own
            ends[coarse, step, part] = lax.ppermute(own, "stn", outward)
            if index < early:
                crossed[coarse, step, part] = lax.ppermute(own, "stn", across)
        power = sum(
            jnp.stack([jnp.concatenate([powers[coarse, step, part] for part in parts[coarse]]) for step in range(2)])
            for coarse in range(coarse_dev)
        )
        power = lax.psum(power, "chan")
        beyond = lax.ppermute(power, "stn", across)
        beyond, *held = lax.optimization_barrier((beyond, *[formed[key] for key in keys[early:]]))
        for index, value in enumerate(held, early):
            crossed[keys[index]] = lax.ppermute(value, "stn", across)
        both = jnp.stack([power, beyond])
        from_inner = lax.ppermute(both, "stn", outward)
        flag = jnp.where(inner, 0, 1)
        odd = own_index % 2 == 1
        from_inner, *held = lax.optimization_barrier((from_inner, *[ends[key] for key in keys]))
        ends = dict(zip(keys, held))
        both = jnp.where(inner, both, from_inner)
        power = jnp.where(side == 0, both, both[::-1]).reshape((groups,) + power.shape[1:])
        left_scale, right_scale = scales(place_power(power), denominator, frames, own_index, tiles)
        far_ends, lefts = {}, {}

        def forward(index):
            far_ends[keys[index]] = lax.ppermute(crossed[keys[index]], "stn", outward)

        def near_work(out, coarse, part):
            lefts[coarse, part] = jnp.where(
                inner,
                jnp.where(odd, formed[coarse, 1, part], formed[coarse, 0, part]),
                jnp.where(odd, ends[coarse, 1, part], ends[coarse, 0, part]),
            )
            near = [(formed[coarse, step, part], ends[coarse, step, part], flag) for step in range(2)]
            return correlate(
                out, lefts[coarse, part], near, left_scale, right_scale, coarse, coarse_dev,
                2 * side, pols, part[0],
            )

        def far_work(out, coarse, step, part):
            far = [(crossed[coarse, step, part], far_ends[coarse, step, part], flag)]
            return correlate(
                out, lefts[coarse, part], far, left_scale, right_scale, coarse, coarse_dev,
                2 * (1 - side) + step, pols, part[0],
            )

        work = [(near_work, (coarse, part)) for coarse in range(coarse_dev) for part in parts[coarse]]
        work += [(far_work, key) for key in keys]
        for index in range(early):
            forward(index)
        for index, (make, which) in enumerate(work):
            out = make(out, *which)
            sent = index + early
            if sent < len(keys):
                out, crossed[keys[sent]] = lax.optimization_barrier((out, crossed[keys[sent]]))
                forward(sent)
    out = out.reshape(2, coarse_dev, own_count, STATIONS, beams, pols, tiles, pols, LANES)
    out = jnp.swapaxes(out, -3, -2).reshape(2, coarse_dev, own_count, STATIONS, beams, pols, pols, fine)
    return out[None]


def solution(mesh):
    in_specs = (
        P(None, "chan", "stn", "tm", None, None),
        P(),
        P("stn"),
        P("stn"),
        P(None, None, "chan", None),
    )
    out_specs = P("tm", None, "chan", "stn", None, None, None, None, None)
    return jax.shard_map(
        per_device, mesh=mesh, in_specs=in_specs, out_specs=out_specs, check_vma=False
    )
```

```python
import jax
import jax.numpy as jnp
from jax import lax
from jax.experimental import pallas as pl
from jax.experimental.pallas import tpu as pltpu
from jax.sharding import PartitionSpec as P


STATIONS = 32
COARSE = 8
LANES = 128
UNROLL = 8
PREPARE = 4
PAIRS = (2, 4)

epsilon = 1e-06


def shifted(value, axis, steps):
    count = lax.axis_size(axis)
    first, last = (max(0, -steps), min(count, count - steps))
    return lax.ppermute(value, axis, [(source, source + steps) for source in range(first, last)])


def dft_tables(length):
    bin_index = jnp.arange(length, dtype=jnp.int32)
    phase_step = bin_index[:, None] * bin_index[None, :] % length
    angles = phase_step.astype(jnp.float32) * (2.0 * jnp.pi / length)
    return (jnp.cos(angles).astype(jnp.bfloat16), jnp.sin(angles).astype(jnp.bfloat16))


def block_ranks(station_map, block_stations, share):
    block = station_map // block_stations
    position = jnp.arange(station_map.shape[-1], dtype=jnp.int32)
    same = block[..., :, None] == block[..., None, :]
    before = position[None, :] < position[:, None]
    return block * share + jnp.sum((same & before).astype(jnp.int32), axis=-1)


def sort_dishes(voltages, order, coarse, parts, share):
    comps, _, _, frames, pols, fine = voltages.shape
    tiles = fine // LANES

    def body(order_ref, x_ref, *refs):
        outs, sems = refs[: len(parts)], refs[len(parts) :]

        def issue(place, carry):
            for part, out_ref, sem in zip(parts, outs, sems):
                dish = order_ref[part * share + place]
                for tile in range(tiles):
                    lanes = pl.ds(tile * LANES, LANES)
                    pltpu.make_async_copy(
                        x_ref.at[:, coarse, dish, :, :, lanes], out_ref.at[:, :, tile, place], sem
                    ).start()
            return carry

        lax.fori_loop(0, share, issue, 0)
        for out_ref, sem in zip(outs, sems):
            pltpu.make_async_copy(out_ref, out_ref, sem).wait()

    results = pl.pallas_call(
        body,
        out_shape=[jax.ShapeDtypeStruct((comps, frames, tiles, share, pols, LANES), voltages.dtype)] * len(parts),
        in_specs=[pl.BlockSpec(memory_space=pltpu.SMEM), pl.BlockSpec(memory_space=pl.ANY)],
        out_specs=[pl.BlockSpec(memory_space=pltpu.VMEM)] * len(parts),
        scratch_shapes=[pltpu.SemaphoreType.DMA] * len(parts),
        name="sort_dishes",
    )(order, voltages)

    return [array.reshape(comps, frames, tiles, share * pols, LANES) for array in results]


def beam_sums(weights, sources, frames_step=4):
    comps, frames, tiles, rows, _ = sources[0].shape
    out_rows, contract = weights.shape

    def body(w_ref, *refs):
        out_ref = refs[-1]
        for frame in range(frames_step):
            pieces = []
            for ref in refs[:-1]:
                for comp in range(comps):
                    pieces.append(jnp.concatenate([ref[comp, frame, t] for t in range(tiles)], axis=1))
            stacked = jnp.concatenate(pieces, axis=0)
            out_ref[frame] = jnp.dot(
                w_ref[...], stacked, preferred_element_type=jnp.float32
            ).astype(out_ref.dtype)

    return pl.pallas_call(
        body,
        grid=(frames // frames_step,),
        in_specs=[pl.BlockSpec((out_rows, contract), lambda i: (0, 0))]
        + [pl.BlockSpec((comps, frames_step, tiles, rows, LANES), lambda i: (0, i, 0, 0, 0))] * len(sources),
        out_specs=pl.BlockSpec((frames_step, out_rows, tiles * LANES), lambda i: (i, 0, 0)),
        out_shape=jax.ShapeDtypeStruct((frames, out_rows, tiles * LANES), jnp.bfloat16),
        name="beam_sums",
    )(weights, *sources)


def channelize(previous, current, taps, cosine, sine, beams):
    frames, out_rows, fine = current.shape
    taps_count = taps.shape[0]
    history = taps_count - 1
    rows = out_rows // (2 * beams)
    tiles = fine // LANES
    previous = previous.reshape(frames, 2, beams * rows, fine)
    current = current.reshape(frames, 2, beams * rows, fine)
    wide_taps = jnp.broadcast_to(taps[:, None, :], (taps_count, 8, fine))

    def body(prev_ref, cur_ref, taps_ref, cos_ref, sin_ref, out_ref, pow_ref, wide_ref, filt_ref):
        for frame in range(history):
            wide_ref[frame] = prev_ref[frames - history + frame].astype(jnp.float32)
        for frame in range(frames):
            wide_ref[history + frame] = cur_ref[frame].astype(jnp.float32)
        for comp in range(2):
            for tile in range(tiles):
                lanes = slice(tile * LANES, (tile + 1) * LANES)
                for low in range(0, rows, 8):
                    for frame in range(frames):
                        terms = [
                            taps_ref[tap, :, lanes]
                            * wide_ref[history + frame - tap, comp, low : low + 8, lanes]
                            for tap in range(taps_count)
                        ]
                        while len(terms) > 1:
                            terms = [
                                a + b for a, b in zip(terms[::2], terms[1::2])
                            ] + terms[len(terms) // 2 * 2 :]
                        filt_ref[comp, frame * rows + low : frame * rows + low + 8, lanes] = terms[0]
        real_part = filt_ref[0].astype(jnp.bfloat16)
        imag_part = filt_ref[1].astype(jnp.bfloat16)

        def dot(a, b):
            return jnp.dot(a, b, preferred_element_type=jnp.float32)

        spec_re = dot(real_part, cos_ref[...]) + dot(imag_part, sin_ref[...])
        spec_im = dot(imag_part, cos_ref[...]) - dot(real_part, sin_ref[...])
        power = jnp.zeros((rows, LANES), jnp.float32)
        for comp, spectrum in enumerate((spec_re, spec_im)):
            rounded = spectrum.astype(jnp.bfloat16)
            squares = rounded.astype(jnp.float32)
            squares = squares * squares
            for tile in range(tiles):
                lanes = slice(tile * LANES, (tile + 1) * LANES)
                for frame in range(frames):
                    out_ref[0, comp, frame, tile * rows : (tile + 1) * rows, :] = rounded[
                        frame * rows : (frame + 1) * rows, lanes
                    ]
                    power = power + squares[frame * rows : (frame + 1) * rows, lanes]
        pow_ref[0] = power

    return pl.pallas_call(
        body,
        grid=(beams,),
        in_specs=[
            pl.BlockSpec((frames, 2, rows, fine), lambda b: (0, 0, b, 0)),
            pl.BlockSpec((frames, 2, rows, fine), lambda b: (0, 0, b, 0)),
            pl.BlockSpec((taps_count, 8, fine), lambda b: (0, 0, 0)),
            pl.BlockSpec((fine, fine), lambda b: (0, 0)),
            pl.BlockSpec((fine, fine), lambda b: (0, 0)),
        ],
        out_specs=[
            pl.BlockSpec((1, 2, frames, tiles * rows, LANES), lambda b: (b, 0, 0, 0, 0)),
            pl.BlockSpec((1, rows, LANES), lambda b: (b, 0, 0)),
        ],
        out_shape=[
            jax.ShapeDtypeStruct((beams, 2, frames, tiles * rows, LANES), jnp.bfloat16),
            jax.ShapeDtypeStruct((beams, rows, LANES), jnp.float32),
        ],
        scratch_shapes=[
            pltpu.VMEM((history + frames, 2, rows, fine), jnp.float32),
            pltpu.VMEM((2, frames * rows, fine), jnp.float32),
        ],
        name="channelize",
    )(previous, current, wide_taps, cosine, sine)


def spread_matrix(stations, pols, tiles, left):
    shape = (stations, pols, tiles, pols)
    station, p, tile, q = (lax.broadcasted_iota(jnp.int32, shape, axis).reshape(-1) for axis in range(4))
    source = (tile * stations + station) * pols + (p if left else q)
    column = jnp.arange(tiles * stations * pols, dtype=jnp.int32)
    return (source[:, None] == column[None, :]).astype(jnp.bfloat16)


def correlate(out, left, rights, left_scale, right_scale, coarse, coarse_count, block, pols, low_beam=0):
    some_beams, _, frames, rows, _ = left.shape
    beams, own, unit, _ = left_scale.shape
    stations = right_scale.shape[1]
    tiles = unit // (pols * pols)
    blocks = len(rights)
    others = own * blocks
    size = own * unit
    spread_left = spread_matrix(own, pols, tiles, True)
    spread_right = spread_matrix(own, pols, tiles, False)
    pair_left, pair_right = PAIRS
    choice = [right if isinstance(right, tuple) else (right,) for right in rights]
    flag = next((right[2] for right in choice if len(right) == 3), 0)
    arrays = [array for right in choice for array in right[:2]]
    scalars = jnp.stack([jnp.asarray(block, jnp.int32), jnp.asarray(flag, jnp.int32)])

    def body(scalar_ref, *refs):
        left_ref, sl_ref, pl_ref, pr_ref = refs[:4]
        right_refs = list(refs[4 : 4 + len(arrays)])
        sr_ref = refs[4 + len(arrays)]
        out_ref, l_ref, r_ref = refs[-3:]

        def spread(matrix_ref, pieces, scale):
            wide = jnp.dot(
                matrix_ref[...], jnp.concatenate(pieces, axis=1), preferred_element_type=jnp.float32
            )
            return [wide[:, i * LANES : (i + 1) * LANES] * scale for i in range(len(pieces))]

        def chosen(index, frame):
            place = sum(min(len(c), 2) for c in choice[:index])
            halves = [right_refs[place][0, o, frame] for o in range(2)]
            if len(choice[index]) == 3:
                second = right_refs[place + 1]
                halves = [jnp.where(scalar_ref[1] == 0, halves[o], second[0, o, frame]) for o in range(2)]
            return halves

        span = PREPARE
        left_scales = sl_ref[0].reshape(size, LANES)
        for first in range(0, frames, span):
            those = range(first, first + span)
            parts = spread(pl_ref, [left_ref[0, o, f] for f in those for o in range(2)], left_scales)
            for frame in those:
                real, imag = parts[2 * (frame - first)], parts[2 * (frame - first) + 1]
                l_ref[frame, 0] = real
                l_ref[frame, 1] = imag
                l_ref[frame, 2] = real + imag
        for index in range(blocks):
            low, high = index * size, (index + 1) * size
            scale = sr_ref[0, index * own : (index + 1) * own].reshape(size, LANES)
            for first in range(0, frames, span):
                those = range(first, first + span)
                parts = spread(pr_ref, [half for f in those for half in chosen(index, f)], scale)
                for frame in those:
                    real, imag = parts[2 * (frame - first)], parts[2 * (frame - first) + 1]
                    r_ref[frame, 0, low:high] = real
                    r_ref[frame, 1, low:high] = imag
                    r_ref[frame, 2, low:high] = real - imag

        left_groups = own // pair_left

        def products(step, carry):
            first_left = (step % left_groups) * pair_left
            first_right = (step // left_groups) * pair_right
            pairs = [(i, j) for i in range(pair_left) for j in range(pair_right)]

            def add_frame(frame, sums):
                lefts = [
                    [l_ref[frame, k, pl.ds((first_left + i) * unit, unit)] for k in range(3)]
                    for i in range(pair_left)
                ]
                result = []
                for j in range(pair_right):
                    right = [r_ref[frame, k, pl.ds((first_right + j) * unit, unit)] for k in range(3)]
                    for i in range(pair_left):
                        for k in range(3):
                            result.append(sums[(j * pair_left + i) * 3 + k] + lefts[i][k] * right[k])
                return tuple(result)

            zeros = tuple(jnp.zeros((unit, LANES), jnp.float32) for _ in range(3 * len(pairs)))
            sums = lax.fori_loop(0, frames, add_frame, zeros, unroll=UNROLL)
            for i, j in pairs:
                rr, ii, mixed = sums[(j * pair_left + i) * 3 : (j * pair_left + i) * 3 + 3]
                out_ref[0, 0, first_left + i, first_right + j, 0] = rr + ii
                out_ref[1, 0, first_left + i, first_right + j, 0] = mixed - rr + ii
            return carry

        lax.fori_loop(0, left_groups * (others // pair_right), products, 0)

    beam_spec = pl.BlockSpec((1, 2, frames, rows, LANES), lambda b, s: (b, 0, 0, 0, 0))
    operands = [left, left_scale, spread_left, spread_right, *arrays, right_scale]
    in_specs = [
        beam_spec,
        pl.BlockSpec((1, own, unit, LANES), lambda b, s: (low_beam + b, 0, 0, 0)),
        pl.BlockSpec(spread_left.shape, lambda b, s: (0, 0)),
        pl.BlockSpec(spread_right.shape, lambda b, s: (0, 0)),
        *[beam_spec for _ in arrays],
        pl.BlockSpec((1, others, unit, LANES), lambda b, s: (low_beam + b, s[0] // blocks, 0, 0)),
    ]
    aliases = {}
    if out is not None:
        aliases = {1 + len(operands): 0}
        operands.append(out)
        in_specs.append(pl.BlockSpec(memory_space=pl.ANY))
    shape = (2, coarse_count, own, stations, beams, unit, LANES)
    return pl.pallas_call(
        body,
        grid_spec=pltpu.PrefetchScalarGridSpec(
            num_scalar_prefetch=1,
            grid=(some_beams,),
            in_specs=in_specs,
            out_specs=pl.BlockSpec(
                (2, 1, own, others, 1, unit, LANES),
                lambda b, s: (0, coarse, 0, s[0] // blocks, low_beam + b, 0, 0),
            ),
            scratch_shapes=[
                pltpu.VMEM((frames, 3, size, LANES), jnp.float32),
                pltpu.VMEM((frames, 3, others * unit, LANES), jnp.float32),
            ],
        ),
        out_shape=jax.ShapeDtypeStruct(shape, jnp.float32),
        input_output_aliases=aliases,
    )(scalars, *operands)


def block_weights(maps, weight_table, target, block_stations, share, pols):
    stations, rows = maps[:, 0], maps[:, 1]
    groups = maps.shape[0]
    _, table_rows, coarse, beams = weight_table.shape
    ranks = block_ranks(stations, block_stations, share)
    place = target * share + jnp.arange(share, dtype=jnp.int32)
    chosen = ranks[:, None, :] == place[None, :, None]
    station = jnp.sum(jnp.where(chosen, stations[:, None, :], 0), axis=-1) - target * block_stations
    row = jnp.sum(jnp.where(chosen, rows[:, None, :], 0), axis=-1)
    columns = (groups, 2, share, pols)
    out_rows = (2, beams, block_stations, pols)
    station = jnp.broadcast_to(station[:, None, :, None], columns).reshape(1, -1)
    row = jnp.broadcast_to(row[:, None, :, None], columns).reshape(1, -1)
    part, pol = (lax.broadcasted_iota(jnp.int32, columns, axis).reshape(1, -1) for axis in (1, 3))
    own_station, own_pol = (lax.broadcasted_iota(jnp.int32, out_rows, axis).reshape(-1, 1) for axis in (2, 3))
    term = jnp.arange(2 * table_rows, dtype=jnp.int32)[:, None]
    hot = (term == part * table_rows + row).astype(jnp.bfloat16)
    kept = (station == own_station) & (pol == own_pol)
    real, imag = weight_table[0], weight_table[1]
    mixing = jnp.stack([jnp.concatenate([real, -imag]), jnp.concatenate([imag, real])])
    result = []
    for channel in range(coarse):
        table = mixing[:, :, channel].swapaxes(1, 2)[:, :, None, None]
        table = jnp.broadcast_to(table, out_rows + (2 * table_rows,)).reshape(-1, 2 * table_rows)
        values = jnp.dot(table, hot, preferred_element_type=jnp.float32)
        result.append(jnp.where(kept, values, 0.0).astype(jnp.bfloat16))
    return result


def scales(power, denominator, frames, own_index, tiles):
    inverse = lax.rsqrt(power / denominator + epsilon)
    blocks, beams, own_count, pols = inverse.shape
    inverse = jnp.moveaxis(inverse, 1, 0).reshape(beams, blocks * own_count, pols)
    full = (beams, blocks * own_count, pols, tiles, pols, LANES)
    unit = pols * tiles * pols
    right = jnp.broadcast_to(inverse[:, :, None, None, :, None] / frames, full)
    mine = lax.dynamic_slice_in_dim(inverse, own_index * own_count, own_count, 1)
    left = jnp.broadcast_to(mine[:, :, :, None, None, None], (beams, own_count) + full[2:])
    return left.reshape(beams, own_count, unit, LANES), right.reshape(beams, blocks * own_count, unit, LANES)


def beam_parts(beams):
    half = beams // 2
    return [(0, half), (half, beams - half)]


def per_device(voltages, fir_taps, station_map, beam_index, weight_table):
    _, coarse_dev, dishes_dev, frames, pols, fine = voltages.shape
    groups = lax.axis_size("stn")
    own_index = lax.axis_index("stn")
    beams = weight_table.shape[3]
    share = dishes_dev // groups
    own_count = STATIONS // groups
    tiles = fine // LANES
    denominator = COARSE * frames * fine
    cosine, sine = dft_tables(fine)
    places = jnp.arange(dishes_dev, dtype=jnp.int32)
    line = groups == 4
    side = own_index // 2 if line else 0
    ranks = block_ranks(station_map, own_count, share)
    ranks = (ranks + 2 * side * share) % dishes_dev
    order = jnp.sum(jnp.where(ranks[None, :] == places[:, None], places[None, :], 0), axis=1)
    maps = jnp.stack([station_map, beam_index])

    def form(weights, sources, beams):
        sums = beam_sums(weights, sources)
        earlier = shifted(sums, "tm", 1)
        formed, lane_power = channelize(earlier, sums, fir_taps, cosine, sine, beams)
        return formed, jnp.sum(lane_power, axis=-1)

    def place_power(power):
        return power.reshape(groups, beams, own_count, pols)

    out = None
    if not line:
        maps = lax.all_gather(maps, "stn")
        weights = block_weights(maps, weight_table, own_index, own_count, share, pols)
        formed, power = [], 0.0
        for coarse in range(coarse_dev):
            blocks = jnp.stack(sort_dishes(voltages, order, coarse, range(groups), share))
            arrived = lax.all_to_all(blocks, "stn", 0, 0, tiled=True)
            own, more = form(weights[coarse], [arrived[g] for g in range(groups)], beams)
            power = power + more
            formed.append((own, lax.all_gather(own, "stn")))
        power = place_power(lax.psum(lax.all_gather(power, "stn"), "chan"))
        left_scale, right_scale = scales(power, denominator, frames, own_index, tiles)
        for coarse in range(coarse_dev):
            own, everyone = formed[coarse]
            rights = [everyone[g] for g in range(groups)]
            out = correlate(out, own, rights, left_scale, right_scale, coarse, coarse_dev, 0, pols)
    else:
        inward, across, outward = [(0, 1), (3, 2)], [(1, 2), (2, 1)], [(1, 0), (2, 3)]
        beyond_one = [(0, 2), (3, 1)]
        inner = (own_index == 1) | (own_index == 2)
        paths = (inward, across, beyond_one)
        known = [maps]
        for path in paths:
            known.append(lax.ppermute(maps, "stn", path))
        maps = jnp.stack(known)
        parts = [beam_parts(beams) for _ in range(coarse_dev)]
        steps = [(coarse, step) for coarse in range(coarse_dev) for step in range(2)]
        arrived = []
        for coarse, step in steps:
            index = len(arrived)
            near, far = sort_dishes(voltages, order, coarse, (step, 2 + step), share)
            sources = [near]
            for sent, path in zip((near, far, far), paths):
                sources.append(lax.ppermute(sent, "stn", path))
            arrived.append(sources)
        formed, ends, powers = {}, {}, {}
        keys = [(coarse, step, part) for coarse, step in steps for part in parts[coarse]]
        early = len(parts[0])
        weights = {}
        for step in range(2):
            for part in {part: None for some in parts for part in some}:
                table = weight_table[..., part[0] : sum(part)]
                weights[step, part] = block_weights(maps, table, 2 * side + step, own_count, share, pols)
        crossed = {}
        for index, (coarse, step, part) in enumerate(keys):
            sources = arrived[steps.index((coarse, step))]
            if index:
                _, sources = lax.optimization_barrier((formed[keys[index - 1]], sources))
            own, powers[coarse, step, part] = form(weights[step, part][coarse], sources, part[1])
            formed[coarse, step, part] = own
            ends[coarse, step, part] = lax.ppermute(own, "stn", outward)
            if index < early:
                crossed[coarse, step, part] = lax.ppermute(own, "stn", across)
        power = sum(
            jnp.stack([jnp.concatenate([powers[coarse, step, part] for part in parts[coarse]]) for step in range(2)])
            for coarse in range(coarse_dev)
        )
        power = lax.psum(power, "chan")
        beyond = lax.ppermute(power, "stn", across)
        beyond, *held = lax.optimization_barrier((beyond, *[formed[key] for key in keys[early:]]))
        for index, value in enumerate(held, early):
            crossed[keys[index]] = lax.ppermute(value, "stn", across)
        both = jnp.stack([power, beyond])
        from_inner = lax.ppermute(both, "stn", outward)
        flag = jnp.where(inner, 0, 1)
        odd = own_index % 2 == 1
        from_inner, *held = lax.optimization_barrier((from_inner, *[ends[key] for key in keys]))
        ends = dict(zip(keys, held))
        both = jnp.where(inner, both, from_inner)
        power = jnp.where(side == 0, both, both[::-1]).reshape((groups,) + power.shape[1:])
        left_scale, right_scale = scales(place_power(power), denominator, frames, own_index, tiles)
        far_ends, lefts = {}, {}

        def forward(index):
            far_ends[keys[index]] = lax.ppermute(crossed[keys[index]], "stn", outward)

        def near_work(out, coarse, part):
            lefts[coarse, part] = jnp.where(
                inner,
                jnp.where(odd, formed[coarse, 1, part], formed[coarse, 0, part]),
                jnp.where(odd, ends[coarse, 1, part], ends[coarse, 0, part]),
            )
            near = [(formed[coarse, step, part], ends[coarse, step, part], flag) for step in range(2)]
            return correlate(
                out, lefts[coarse, part], near, left_scale, right_scale, coarse, coarse_dev,
                2 * side, pols, part[0],
            )

        def far_work(out, coarse, step, part):
            far = [(crossed[coarse, step, part], far_ends[coarse, step, part], flag)]
            return correlate(
                out, lefts[coarse, part], far, left_scale, right_scale, coarse, coarse_dev,
                2 * (1 - side) + step, pols, part[0],
            )

        work = [(near_work, (coarse, part)) for coarse in range(coarse_dev) for part in parts[coarse]]
        work += [(far_work, key) for key in keys]
        for index in range(early):
            forward(index)
        for index, (make, which) in enumerate(work):
            out = make(out, *which)
            sent = index + early
            if sent < len(keys):
                out, crossed[keys[sent]] = lax.optimization_barrier((out, crossed[keys[sent]]))
                forward(sent)
    out = out.reshape(2, coarse_dev, own_count, STATIONS, beams, pols, tiles, pols, LANES)
    out = jnp.swapaxes(out, -3, -2).reshape(2, coarse_dev, own_count, STATIONS, beams, pols, pols, fine)
    return out[None]


def solution(mesh):
    in_specs = (
        P(None, "chan", "stn", "tm", None, None),
        P(),
        P("stn"),
        P("stn"),
        P(None, None, "chan", None),
    )
    out_specs = P("tm", None, "chan", "stn", None, None, None, None, None)
    return jax.shard_map(
        per_device, mesh=mesh, in_specs=in_specs, out_specs=out_specs, check_vma=False
    )
```
